8 devices in a mesh: dp: 2 (over z, y), ep: 4 (over x, core).
Axes of the slice: x: 2, y: 2, z: 1, core: 2. Of those that a mesh axis runs over, the one named last changes fastest.
Arguments:
- h0: bfloat16 [8, 256, 2048], P(('dp', 'ep')), parts along dimension 0
- idx: int32 [8, 256, 6], P(('dp', 'ep')), parts along dimension 0
- slot: int32 [8, 256, 6], P(('dp', 'ep')), parts along dimension 0
- ln_attn: bfloat16 [2048], replicated
- wq: bfloat16 [2048, 2048], replicated
- wk: bfloat16 [2048, 2048], replicated
- wv: bfloat16 [2048, 2048], replicated
- wo: bfloat16 [2048, 2048], replicated
- ln_ffn: bfloat16 [2048], replicated
- ws1: bfloat16 [2048, 2816], replicated
- ws3: bfloat16 [2048, 2816], replicated
- ws2: bfloat16 [2816, 2048], replicated
- ln_moe: bfloat16 [2048], replicated
- wr: bfloat16 [2048, 64], replicated
- ue1: bfloat16 [64, 2048, 1408], P('ep')
- ue3: bfloat16 [64, 2048, 1408], P('ep')
- ue2: bfloat16 [64, 1408, 2048], P('ep')
Outputs:
- output: bfloat16 [8, 256, 2048], P(('dp', 'ep')), parts along dimension 0
There are 2 independent parts. The reference program is written for one: setup_inputs(seed, part) draws one part's arguments, and reference() takes and returns one part's arrays. A program takes and returns all parts, laid end to end along the dimension named above; an argument that names none is the same for every part.
All inputs are finite; a program needn't handle non-finite values.
Results may differ from the reference program's by a relative error of at most 0.00930081.
Values are sent between devices in bfloat16 or wider.
A program may use at most 1.5 GiB of HBM per device.

```python
import jax
import jax.numpy as jnp
from jax import lax

D = 2048
HEADS = 16
HEAD = 128
EXPERTS = 64
TOP = 6
FE = 1408
FS = 2816
SEQ = 256
SEQS = 1
G = 4
CAP = 48

T = SEQS * SEQ
EPS = 1e-6


def _dot(a, b):
    return jnp.dot(a, b, preferred_element_type=jnp.float32)


def _rms(x, w):
    xf = x.astype(jnp.float32)
    r = lax.rsqrt(jnp.mean(xf * xf, axis=-1, keepdims=True) + EPS)
    return (xf * r * w.astype(jnp.float32)).astype(jnp.bfloat16)


def _rope(x):
    half = HEAD // 2
    freq = 10000.0 ** (-jnp.arange(half, dtype=jnp.float32) / half)
    ang = jnp.arange(SEQ, dtype=jnp.float32)[:, None] * freq[None, :]
    c = jnp.cos(ang)[:, None, :]
    s = jnp.sin(ang)[:, None, :]
    x1, x2 = x[..., :half], x[..., half:]
    return jnp.concatenate([x1 * c - x2 * s, x2 * c + x1 * s], axis=-1)


def _normal(key, shape, scale):
    return (jax.random.normal(key, shape, jnp.float32) * scale).astype(jnp.bfloat16)


def _scale(key):
    return jax.random.uniform(key, (D,), jnp.float32, 0.8, 1.2).astype(jnp.bfloat16)


def _expert_weight(weight_key):
    levels = jnp.sum(jax.random.randint(weight_key, (9, EXPERTS), 0, 10, jnp.int32), axis=0)
    hot_bias = 12 * (jnp.arange(EXPERTS) < EXPERTS // G).astype(jnp.int32)
    quarter = jnp.maximum(levels + hot_bias - 16, 0)
    return jnp.left_shift(4 + quarter % 4, quarter // 4).astype(jnp.int32)


def _route(route_key, weight):
    draw_rows = jax.random.bits(route_key, (T, TOP), jnp.uint32)

    def step(counts, draw_row):
        open_weight = jnp.where(counts < CAP, weight, 0).astype(jnp.int32)
        picked_list = []
        for choice in range(TOP):
            cumulative = jnp.cumsum(open_weight)
            total_weight = cumulative[-1].astype(jnp.uint32)
            target_val = (draw_row[choice] % total_weight).astype(jnp.int32)
            pick_id = jnp.searchsorted(cumulative, target_val, side='right').astype(jnp.int32)
            picked_list.append(pick_id)
            open_weight = open_weight.at[pick_id].set(0)
        chosen = jnp.stack(picked_list)
        return counts.at[chosen].add(1), (chosen, counts[chosen])

    _, (chosen, slots) = lax.scan(step, jnp.zeros((EXPERTS,), jnp.int32), draw_rows)
    return chosen.astype(jnp.int32), slots.astype(jnp.int32)


def setup_inputs(seed: int = 0, part: int = 0) -> dict:
    key = jax.random.PRNGKey(seed)
    kh, kr = jax.random.split(jax.random.fold_in(key, part))
    ks = jax.random.split(key, 15)
    hd = HEADS * HEAD
    expert_weight = _expert_weight(jax.random.fold_in(ks[14], 7))
    idx, slot = jax.vmap(lambda k: _route(k, expert_weight))(jax.random.split(kr, G))
    return {
        'h0': _normal(kh, (G * SEQS, SEQ, D), 1.0),
        'idx': idx.reshape(G * SEQS, SEQ, TOP),
        'slot': slot.reshape(G * SEQS, SEQ, TOP),
        'ln_attn': _scale(ks[0]),
        'wq': _normal(ks[1], (D, hd), 1.5 * D ** -0.5),
        'wk': _normal(ks[2], (D, hd), 1.5 * D ** -0.5),
        'wv': _normal(ks[3], (D, hd), D ** -0.5),
        'wo': _normal(ks[4], (hd, D), hd ** -0.5),
        'ln_ffn': _scale(ks[5]),
        'ws1': _normal(ks[6], (D, FS), D ** -0.5),
        'ws3': _normal(ks[7], (D, FS), D ** -0.5),
        'ws2': _normal(ks[8], (FS, D), FS ** -0.5),
        'ln_moe': _scale(ks[9]),
        'wr': _normal(ks[10], (D, EXPERTS), 1.5 * D ** -0.5),
        'ue1': _normal(ks[11], (EXPERTS, D, FE), D ** -0.5),
        'ue3': _normal(ks[12], (EXPERTS, D, FE), D ** -0.5),
        'ue2': _normal(ks[13], (EXPERTS, FE, D), 2.0 * FE ** -0.5),
    }


def reference(h0, idx, slot, ln_attn, wq, wk, wv, wo, ln_ffn, ws1, ws3, ws2, ln_moe, wr, ue1, ue3, ue2):
    nb = h0.shape[0]
    n = nb * SEQ
    x1 = _rms(h0, ln_attn)
    causal = jnp.arange(SEQ)[:, None] >= jnp.arange(SEQ)[None, :]

    def attn(xs):
        q = _rope(_dot(xs, wq).reshape(SEQ, HEADS, HEAD)).astype(jnp.bfloat16)
        k = _rope(_dot(xs, wk).reshape(SEQ, HEADS, HEAD)).astype(jnp.bfloat16)
        v = _dot(xs, wv).astype(jnp.bfloat16).reshape(SEQ, HEADS, HEAD)
        s = jnp.einsum('qhe,khe->hqk', q.astype(jnp.float32), k.astype(jnp.float32)) * HEAD ** -0.5
        p = jax.nn.softmax(jnp.where(causal[None], s, -1e30), axis=-1).astype(jnp.bfloat16)
        o = jnp.einsum('hqk,khe->qhe', p.astype(jnp.float32), v.astype(jnp.float32))
        return o.astype(jnp.bfloat16).reshape(SEQ, HEADS * HEAD)

    o = lax.map(attn, x1).reshape(n, HEADS * HEAD)
    h = h0.reshape(n, D)
    a = (h.astype(jnp.float32) + _dot(o, wo)).astype(jnp.bfloat16)
    x2 = _rms(a, ln_ffn)
    hs = (jax.nn.silu(_dot(x2, ws1)) * _dot(x2, ws3)).astype(jnp.bfloat16)
    f = _dot(hs, ws2)

    u = _rms(h, ln_moe)
    gi = idx.reshape(n, TOP)
    sl = slot.reshape(n, TOP)
    g = jax.nn.softmax(jnp.take_along_axis(_dot(u, wr), gi, axis=1), axis=-1)
    dev = jnp.arange(n, dtype=jnp.int32) // T
    pos = gi * (G * CAP) + dev[:, None] * CAP + sl
    src = jnp.full((EXPERTS * G * CAP,), n, jnp.int32).at[pos.reshape(-1)].set(
        jnp.arange(n * TOP, dtype=jnp.int32) // TOP)
    u_pad = jnp.concatenate([u, jnp.zeros((1, D), jnp.bfloat16)], axis=0)
    buf = u_pad[src].reshape(EXPERTS, G * CAP, D)

    def expert(args):
        x, w1, w3, w2 = args
        he = (jax.nn.silu(_dot(x, w1)) * _dot(x, w3)).astype(jnp.bfloat16)
        return _dot(he, w2).astype(jnp.bfloat16)

    y = lax.map(expert, (buf, ue1, ue3, ue2)).reshape(EXPERTS * G * CAP, D)
    m = jnp.sum(g[:, :, None] * y[pos].astype(jnp.float32), axis=1)
    out = a.astype(jnp.float32) + f + m
    return out.astype(jnp.bfloat16).reshape(nb, SEQ, D)
```

```python
import jax
import jax.numpy as jnp
import numpy as np
from jax import lax
from jax.experimental import pallas as pl
from jax.experimental.pallas import tpu as pltpu
from jax.sharding import PartitionSpec as P

MESH = pl.DeviceIdType.MESH
F32 = jnp.float32
BF16 = jnp.bfloat16
EPS = 1e-6
HEAD = 128
CAP_FACTOR = 2

OWN, SIB, CROSS, DIAG = range(4)
NA = 4
NB = 6
CC = 512
UC = 4


def _dot(a, b):
    return jnp.dot(a, b, preferred_element_type=F32)


def _rope_tables(s):
    half = HEAD // 2
    freq = np.float32(10000.0) ** (-np.arange(half, dtype=np.float32) / np.float32(half))
    ang = np.arange(s, dtype=np.float32)[:, None] * freq.astype(np.float32)[None, :]
    c, sn = np.cos(ang), np.sin(ang)
    return np.concatenate([c, c], 1).astype(np.float32), np.concatenate([-sn, sn], 1).astype(np.float32)


def _build(t, d, fe, fs, el, cap, top):
    nh = d // HEAD
    rows = 4 * cap
    rl = el * cap
    nch = d // CC
    uc = t // UC
    nta = 8 + 2 * el
    nue2 = nch * el
    nf = fs // fe

    def kernel(h0_hbm, idx_ref, slot_ref, ln_ref, cos_ref, sin_ref, wr_ref, wq, wk, wv, wo, ws1, ws3, ws2,
               ue1, ue3, ue2, out_hbm,
               ring_a, ring_b, u_all, xy, he, hsf, h0v, x1v, mrow, mcol,
               macc, rsib, rcross, rdiag, sdiag, ssib,
               sem_a, sem_b, sem_in, sem_out,
               ms, mr, us_sib, ur_sib, us_cross, ur_cross, us_fwd, ur_diag,
               cs_diag, cr_diag, cs_sib, cr_sib, cs_cross, cr_cross):
        me = lax.axis_index('ep')
        core = lax.rem(me, 2)
        sib = me + 1 - 2 * core
        cross = lax.rem(me + 2, 4)
        diag = lax.rem(sib + 2, 4)
        base = (me * rl).astype(F32)

        def rcopy(src, dst, ssem, rsem, dev):
            return pltpu.make_async_remote_copy(src_ref=src, dst_ref=dst, send_sem=ssem, recv_sem=rsem,
                                                device_id={'ep': dev}, device_id_type=MESH)

        def a_dense(k):
            w = (wq, wk, wv, wo)[k // 2]
            return pltpu.make_async_copy(w.at[:, pl.ds((k % 2) * (d // 2), d // 2)],
                                         ring_a.at[k % NA, :, pl.ds(0, d // 2)], sem_a.at[k % NA])

        def a_expert(e, s):
            return pltpu.make_async_copy((ue1, ue3)[s % 2].at[e], ring_a.at[s], sem_a.at[s])

        def a_shared(k):
            return pltpu.make_async_copy((ws1, ws3)[k % 2].at[:, pl.ds((k // 2) * fe, fe)],
                                         ring_a.at[k], sem_a.at[k])

        def b_ue2(i):
            sl = lax.rem(i, NB)
            return pltpu.make_async_copy(
                ue2.at[lax.rem(i, el), :, pl.ds(pl.multiple_of(lax.div(i, el) * CC, CC), CC)],
                ring_b.at[sl], sem_b.at[sl])

        def b_ws2(i):
            k = i - nue2
            sl = lax.rem(i, NB)
            return pltpu.make_async_copy(
                ws2.at[pl.ds(pl.multiple_of(lax.rem(k, nf) * fe, 128), fe),
                       pl.ds(pl.multiple_of(lax.div(k, nf) * CC, CC), CC)],
                ring_b.at[sl], sem_b.at[sl])

        h0_in = pltpu.make_async_copy(h0_hbm, h0v, sem_in)
        h0_in.start()
        for k in range(NA):
            a_dense(k).start()
        bar = pltpu.get_barrier_semaphore()
        for dev in (sib, cross, diag):
            pl.semaphore_signal(bar, inc=1, device_id={'ep': dev}, device_id_type=MESH)
        pl.semaphore_wait(bar, 3)
        h0_in.wait()

        def u_sib(i):
            r = pl.ds(i * uc, uc)
            return rcopy(u_all.at[OWN, r, pl.ds(0, d)], u_all.at[SIB, r, pl.ds(0, d)], us_sib.at[i], ur_sib.at[i], sib)

        def u_cross(i):
            r = pl.ds(i * uc, uc)
            return rcopy(u_all.at[OWN, r, pl.ds(0, d)], u_all.at[CROSS, r, pl.ds(0, d)],
                         us_cross.at[i], ur_cross.at[i], cross)

        def u_fwd(i):
            r = pl.ds(i * uc, uc)
            return rcopy(u_all.at[CROSS, r, pl.ds(0, d)], u_all.at[DIAG, r, pl.ds(0, d)],
                         us_fwd.at[i], ur_diag.at[i], sib)

        def relay(i):
            u_cross(i).wait_recv()
            u_fwd(i).start()

        for i in range(UC):
            def norm_in(k, _):
                r = pl.ds(pl.multiple_of(i * uc + k * 16, 16), 16)
                x = h0v[r, :].astype(F32)
                n = x * lax.rsqrt(jnp.mean(x * x, axis=-1, keepdims=True) + EPS)
                u_all[OWN, r, 0:d] = (n * ln_ref[2:3, :]).astype(BF16)
                x1v[r, :] = (n * ln_ref[0:1, :]).astype(BF16)
                return 0

            lax.fori_loop(0, uc // 16, norm_in, 0)
            u_cross(i).start()
            u_sib(i).start()

        lg = _dot(u_all[OWN, :, 0:d], wr_ref[...])
        ex = lax.broadcasted_iota(jnp.int32, lg.shape, 1)
        lj = [jnp.sum(jnp.where(ex == idx_ref[:, j:j + 1], lg, 0.0), axis=-1, keepdims=True) for j in range(top)]
        mx = lj[0]
        for j in range(1, top):
            mx = jnp.maximum(mx, lj[j])
        ej = [jnp.exp(v - mx) for v in lj]
        tot = ej[0]
        for j in range(1, top):
            tot = tot + ej[j]
        lane = lax.broadcasted_iota(jnp.int32, (t, 128), 1)
        meta = jnp.zeros((t, 128), F32)
        for j in range(top):
            pos = (idx_ref[:, j:j + 1] * cap + slot_ref[:, j:j + 1]).astype(F32)
            meta = jnp.where(lane == j, pos, meta)
            meta = jnp.where(lane == 8 + j, ej[j] / tot, meta)
        mcol[OWN] = meta
        mrow[OWN] = jnp.transpose(meta)[0:16, :]
        m_copies = [rcopy(mrow.at[OWN], mrow.at[role], ms.at[role - 1], mr.at[role - 1], dev)
                    for role, dev in ((SIB, sib), (CROSS, cross), (DIAG, diag))]
        for c in m_copies:
            c.start()

        def qkv(k, rope):
            a_dense(k).wait()

            def half(n, _):
                y = _dot(x1v[...], ring_a[k % NA, :, pl.ds(pl.multiple_of(n * 512, 512), 512)])
                for h in range(4):
                    yh = y[:, h * HEAD:(h + 1) * HEAD]
                    if rope:
                        yh = yh * cos_ref[...] + pltpu.roll(yh, HEAD // 2, 1) * sin_ref[...]
                    col = pl.multiple_of(n * 512 + ((k % 2) * (d // 2) + h * HEAD), HEAD)
                    xy[(k // 2) * t:(k // 2 + 1) * t, pl.ds(col, HEAD)] = yh.astype(BF16)
                return 0

            lax.fori_loop(0, 2, half, 0)

        for k in range(6):
            qkv(k, k < 4)
            if k < 4:
                a_dense(k + NA).start()
            else:
                a_expert(0, k % NA - 0).start()
        relay(0)
        for i in range(NB):
            b_ue2(i).start()

        ri = lax.broadcasted_iota(jnp.int32, (t, t), 0)
        ci = lax.broadcasted_iota(jnp.int32, (t, t), 1)

        def head_pair(hp, _):
            for s in range(2):
                col = pl.ds(pl.multiple_of((hp * 2 + s) * HEAD, HEAD), HEAD)
                q = xy[0:t, col]
                kk = xy[t:2 * t, col]
                vv = xy[2 * t:3 * t, col]
                sc = lax.dot_general(q, kk, (((1,), (1,)), ((), ())), preferred_element_type=F32) * HEAD ** -0.5
                sc = jnp.where(ri >= ci, sc, -1e30)
                p = jnp.exp(sc - jnp.max(sc, axis=-1, keepdims=True))
                p = (p / jnp.sum(p, axis=-1, keepdims=True)).astype(BF16)
                xy[0:t, col] = _dot(p, vv).astype(BF16)
            return 0

        lax.fori_loop(0, nh // 2, head_pair, 0)
        relay(1)

        for k in (6, 7):
            a_dense(k).wait()

            def half(n, _):
                col = pl.ds(pl.multiple_of((k % 2) * (d // 2) + n * 512, 512), 512)
                y = _dot(xy[0:t, :], ring_a[k % NA, :, pl.ds(pl.multiple_of(n * 512, 512), 512)])
                h0v[:, col] = (h0v[:, col].astype(F32) + y).astype(BF16)
                return 0

            lax.fori_loop(0, 2, half, 0)
            a_expert(1, k % NA).start()

        def norm_a(k, _):
            r = pl.ds(pl.multiple_of(k * 16, 16), 16)
            x = h0v[r, :].astype(F32)
            n = x * lax.rsqrt(jnp.mean(x * x, axis=-1, keepdims=True) + EPS)
            x1v[r, :] = (n * ln_ref[1:2, :]).astype(BF16)
            return 0

        lax.fori_loop(0, t // 16, norm_a, 0)

        for c in m_copies:
            c.wait()
        for role in (SIB, CROSS, DIAG):
            mcol[role] = jnp.transpose(jnp.concatenate([mrow[role], jnp.zeros((112, t), F32)], axis=0))
        for i in range(2, UC):
            relay(i)
        for i in range(UC):
            u_sib(i).wait()
            u_cross(i).wait_send()
            u_fwd(i).wait()

        def group(g, _):
            def gather(role, _):
                rr = (lax.broadcasted_iota(jnp.int32, (rows, t), 0) + g * rows).astype(F32) + base
                hit = rr == mrow[role, 0:1, :]
                for j in range(1, top):
                    hit = hit | (rr == mrow[role, j:j + 1, :])
                oh = jnp.where(hit, 1.0, 0.0).astype(BF16)
                for n in range(d // 512):
                    xg = _dot(oh, u_all[role, :, n * 512:(n + 1) * 512]).astype(BF16)
                    for e4 in range(4):
                        xy[pl.ds(pl.multiple_of(e4 * rows + role * cap, 16), cap), n * 512:(n + 1) * 512] = (
                            xg[e4 * cap:(e4 + 1) * cap, :])
                return 0

            lax.fori_loop(0, 4, gather, 0)

            def pair(pp, _):
                e0 = g * 4 + pp * 2
                for s in range(2):
                    e = e0 + s
                    xr = pl.ds(pl.multiple_of((pp * 2 + s) * rows, 16), rows)
                    hr = pl.ds(pl.multiple_of(e * rows, 16), rows)
                    for w in range(2):
                        sl = 2 * s + w
                        a_expert(e, sl).wait()
                        for n0 in range(0, fe, 512):
                            n1 = min(n0 + 512, fe)
                            y = _dot(xy[xr, :], ring_a[sl, :, n0:n1])
                            if w == 0:
                                hsf[0:rows, n0:n1] = y * jax.nn.sigmoid(y)
                            else:
                                he[hr, n0:n1] = (hsf[0:rows, n0:n1] * y).astype(BF16)

                        @pl.when(e0 + 2 < el)
                        def _():
                            a_expert(e + 2, sl).start()

                        @pl.when(e0 + 2 >= el)
                        def _():
                            a_shared(sl).start()
                return 0

            lax.fori_loop(0, 2, pair, 0)
            return 0

        lax.fori_loop(0, el // 4, group, 0)

        def gates(i, _):
            role = lax.div(i, t // 64)
            r = pl.ds(pl.multiple_of(lax.rem(i, t // 64) * 64, 64), 64)
            for b in range(rl // 256):
                rr = (lax.broadcasted_iota(jnp.int32, (64, 256), 1) + b * 256).astype(F32) + base
                comb = jnp.zeros((64, 256), F32)
                for j in range(top):
                    comb = jnp.where(rr == mcol[role, r, j:j + 1], mcol[role, r, 8 + j:9 + j], comb)
                for part in range(3):
                    piece = comb.astype(BF16)
                    u_all[role, r, part * rl + b * 256:part * rl + (b + 1) * 256] = piece
                    comb = comb - piece.astype(F32)
            return 0

        lax.fori_loop(0, 4 * (t // 64), gates, 0)

        def c_diag(c):
            return rcopy(sdiag.at[lax.rem(c, 2)], rdiag.at[c], cs_diag.at[c], cr_diag.at[c], sib)

        def c_sib(c):
            return rcopy(ssib.at[lax.rem(c, 2)], rsib.at[c], cs_sib.at[c], cr_sib.at[c], sib)

        def c_cross(c):
            return rcopy(rdiag.at[c], rcross.at[c], cs_cross.at[c], cr_cross.at[c], cross)

        def partial(role):
            yc = xy[:, role * CC:(role + 1) * CC]
            return (_dot(u_all[role, :, 0:rl], yc) + _dot(u_all[role, :, rl:2 * rl], yc)
                    + _dot(u_all[role, :, 2 * rl:3 * rl], yc))

        def chunk(c, _):
            def four(q, _):
                for s in range(4):
                    e = q * 4 + s
                    i = c * el + e
                    sl = lax.rem(i, NB)
                    b_ue2(i).wait()
                    y = _dot(he[pl.ds(pl.multiple_of(e * rows, 16), rows), :], ring_b[sl]).astype(BF16)
                    for role in range(4):
                        xy[pl.ds(pl.multiple_of(e * cap, 16), cap), role * CC:(role + 1) * CC] = (
                            y[role * cap:(role + 1) * cap, :])

                    @pl.when(i + NB < nue2)
                    def _():
                        b_ue2(i + NB).start()

                    @pl.when(i + NB >= nue2)
                    def _():
                        b_ws2(i + NB).start()
                return 0

            lax.fori_loop(0, el // 4, four, 0)

            @pl.when(c >= 2)
            def _():
                c_diag(c - 2).wait_send()
                c_sib(c - 2).wait_send()

            sdiag[lax.rem(c, 2)] = partial(DIAG)
            c_diag(c).start()
            ssib[lax.rem(c, 2)] = partial(SIB)
            c_sib(c).start()
            macc[c] = partial(OWN)
            pc = partial(CROSS)
            c_diag(c).wait_recv()
            rdiag[c] = rdiag[c] + pc
            c_cross(c).start()
            return 0

        lax.fori_loop(0, nch, chunk, 0)

        for half in range(nf):
            for w in range(2):
                k = half * 2 + w
                a_shared(k).wait()

                def cols_of(n, width):
                    cols = pl.ds(n, width)
                    y = _dot(x1v[...], ring_a[k, :, cols])
                    if w == 0:
                        hsf[:, cols] = y * jax.nn.sigmoid(y)
                    else:
                        he[half * t:(half + 1) * t, cols] = (hsf[:, cols] * y).astype(BF16)

                def step(n, _):
                    cols_of(pl.multiple_of(n * 512, 512), 512)
                    return 0

                lax.fori_loop(0, fe // 512, step, 0)
                if fe % 512:
                    cols_of(fe - fe % 512, fe % 512)

        def shared_out(c, _):
            for half in range(nf):
                i = nue2 + c * nf + half
                b_ws2(i).wait()
                macc[c] += _dot(he[half * t:(half + 1) * t, :], ring_b[lax.rem(i, NB)])

                @pl.when(i + NB < nue2 + nf * nch)
                def _():
                    b_ws2(i + NB).start()
            return 0

        lax.fori_loop(0, nch, shared_out, 0)
        for c in range(nch):
            cols = slice(c * CC, (c + 1) * CC)
            c_sib(c).wait_recv()
            c_cross(c).wait_recv()

            def fin(k, _):
                r = pl.ds(pl.multiple_of(k * 32, 32), 32)
                x1v[r, cols] = (h0v[r, cols].astype(F32) + macc[c, r] + (rsib[c, r] + rcross[c, r])).astype(BF16)
                return 0

            lax.fori_loop(0, t // 32, fin, 0)
            pltpu.make_async_copy(x1v.at[:, pl.ds(c * CC, CC)], out_hbm.at[:, pl.ds(c * CC, CC)],
                                  sem_out.at[c]).start()
        for c in range(nch):
            if c >= nch - 2:
                c_diag(c).wait_send()
                c_sib(c).wait_send()
            c_cross(c).wait_send()
            pltpu.make_async_copy(x1v.at[:, pl.ds(c * CC, CC)], out_hbm.at[:, pl.ds(c * CC, CC)],
                                  sem_out.at[c]).wait()

    dma = pltpu.SemaphoreType.DMA
    vm = pltpu.VMEM
    any_ = pl.BlockSpec(memory_space=pl.ANY)
    vmem = pl.BlockSpec(memory_space=pltpu.VMEM)
    return pl.pallas_call(
        kernel,
        out_shape=jax.ShapeDtypeStruct((t, d), BF16),
        in_specs=[any_] + [vmem] * 6 + [any_] * 10,
        out_specs=any_,
        scratch_shapes=[
            vm((NA, d, fe), BF16),
            vm((NB, fe, CC), BF16),
            vm((4, t, max(d, 3 * rl)), BF16),
            vm((max(4 * rows, 3 * t, rl), d), BF16),
            vm((el * rows, fe), BF16),
            vm((t, fe), F32),
            vm((t, d), BF16),
            vm((t, d), BF16),
            vm((4, 16, t), F32),
            vm((4, t, 128), F32),
            vm((nch, t, CC), F32),
            vm((nch, t, CC), F32),
            vm((nch, t, CC), F32),
            vm((nch, t, CC), F32),
            vm((2, t, CC), F32),
            vm((2, t, CC), F32),
            dma((NA,)), dma((NB,)), dma, dma((nch,)),
            dma((3,)), dma((3,)),
            dma((UC,)), dma((UC,)), dma((UC,)), dma((UC,)), dma((UC,)), dma((UC,)),
            dma((nch,)), dma((nch,)), dma((nch,)), dma((nch,)), dma((nch,)), dma((nch,)),
        ],
        compiler_params=pltpu.CompilerParams(collective_id=0, has_side_effects=True,
                                             vmem_limit_bytes=67043328),
        name='moe_layer',
    )


def solution(mesh):
    g_ = mesh.shape['ep']
    rows = P(('dp', 'ep'))
    rep = P()

    def local(h0, idx, slot, ln_attn, wq, wk, wv, wo, ln_ffn, ws1, ws3, ws2, ln_moe, wr, ue1, ue3, ue2):
        b, s, d = h0.shape
        top = idx.shape[-1]
        el, _, fe = ue1.shape
        t = b * s
        cap = CAP_FACTOR * t * top // (el * g_)
        lns = jnp.stack([ln_attn, ln_ffn, ln_moe]).astype(F32)
        cos, sin = _rope_tables(s)
        call = _build(t, d, fe, ws1.shape[1], el, cap, top)
        out = call(h0.reshape(t, d), idx.reshape(t, top), slot.reshape(t, top), lns, cos, sin, wr,
                   wq, wk, wv, wo, ws1, ws3, ws2, ue1, ue3, ue2)
        return out.reshape(b, s, d)

    specs = (rows, rows, rows) + (rep,) * 11 + (P('ep'), P('ep'), P('ep'))
    return jax.shard_map(local, mesh=mesh, in_specs=specs, out_specs=rows, check_vma=False)
```

```python
import jax
import jax.numpy as jnp
import numpy as np
from jax import lax
from jax.experimental import pallas as pl
from jax.experimental.pallas import tpu as pltpu
from jax.sharding import PartitionSpec as P

MESH = pl.DeviceIdType.MESH
F32 = jnp.float32
BF16 = jnp.bfloat16
EPS = 1e-6
HEAD = 128
CAP_FACTOR = 2

OWN, SIB, CROSS, DIAG = range(4)
NA = 4
NB = 3
EB = 4
CC = 256
UC = 8


def _dot(a, b):
    return jnp.dot(a, b, preferred_element_type=F32)


def _rope_tables(s):
    half = HEAD // 2
    freq = np.float32(10000.0) ** (-np.arange(half, dtype=np.float32) / np.float32(half))
    ang = np.arange(s, dtype=np.float32)[:, None] * freq.astype(np.float32)[None, :]
    c, sn = np.cos(ang), np.sin(ang)
    return np.concatenate([c, c], 1).astype(np.float32), np.concatenate([-sn, sn], 1).astype(np.float32)


def _build(t, d, fe, fs, el, cap, top):
    nh = d // HEAD
    rows = 4 * cap
    rl = el * cap
    nch = d // CC
    uc = t // UC
    nta = 8 + 2 * el
    nue2 = nch * el // EB
    nf = fs // fe
    cpt = EB // nf
    nws2 = nch // cpt

    def kernel(h0_hbm, idx_ref, slot_ref, lna_ref, lnf_ref, lnm_ref, cos_ref, sin_ref, wr_ref, wq, wk, wv, wo, ws1, ws3, ws2,
               ue1, ue3, ue2, out_hbm,
               ring_a, ring_b, u_all, comb, xy, he, ln_ref, h0v, x1v, mrow, mcol,
               macc, rsib, rcross, rdiag, sdiag, ssib,
               sem_a, sem_b, sem_in, sem_out,
               ms, mr, us_sib, ur_sib, us_cross, ur_cross, us_fwd, ur_diag,
               cs_diag, cr_diag, cs_sib, cr_sib, cs_cross, cr_cross):
        me = lax.axis_index('ep')
        core = lax.rem(me, 2)
        sib = me + 1 - 2 * core
        cross = lax.rem(me + 2, 4)
        diag = lax.rem(sib + 2, 4)
        base = (me * rl).astype(F32)

        def rcopy(src, dst, ssem, rsem, dev):
            return pltpu.make_async_remote_copy(src_ref=src, dst_ref=dst, send_sem=ssem, recv_sem=rsem,
                                                device_id={'ep': dev}, device_id_type=MESH)

        def a_dense(k):
            w = (wq, wk, wv, wo)[k // 2]
            return pltpu.make_async_copy(w.at[:, pl.ds((k % 2) * (d // 2), d // 2)],
                                         ring_a.at[k % NA, :, pl.ds(0, d // 2)], sem_a.at[k % NA])

        def a_expert(e, s):
            return pltpu.make_async_copy((ue1, ue3)[s % 2].at[e], ring_a.at[s], sem_a.at[s])

        def a_shared(k):
            return pltpu.make_async_copy((ws1, ws3)[k % 2].at[:, pl.ds((k // 2) * fe, fe)],
                                         ring_a.at[k], sem_a.at[k])

        def b_ue2(i):
            sl = lax.rem(i, NB)
            e0 = lax.rem(i, el // EB) * EB
            col = pl.multiple_of(lax.div(i, el // EB) * CC, CC)
            return pltpu.make_async_copy(ue2.at[pl.ds(e0, EB), :, pl.ds(col, CC)], ring_b.at[sl], sem_b.at[sl, 0])

        def b_ws2(i):
            sl = lax.rem(i, NB)
            k = i - nue2
            return [pltpu.make_async_copy(
                ws2.at[pl.ds(half * fe, fe), pl.ds(pl.multiple_of((k * cpt + u) * CC, CC), CC)],
                ring_b.at[sl, u * nf + half], sem_b.at[sl, u * nf + half])
                for u in range(cpt) for half in range(nf)]

        h0_in = pltpu.make_async_copy(h0_hbm, h0v, sem_in)
        h0_in.start()
        bar = pltpu.get_barrier_semaphore()
        for dev in (sib, cross, diag):
            pl.semaphore_signal(bar, inc=1, device_id={'ep': dev}, device_id_type=MESH)
        for k, ref in enumerate((lna_ref, lnf_ref, lnm_ref)):
            w = ref[...].astype(F32)
            for i in range(d // 128):
                ln_ref[k:k + 1, i * 128:(i + 1) * 128] = w[i:i + 1, :]
        h0_in.wait()
        for k in range(NA):
            a_dense(k).start()

        def u_sib(i):
            r = pl.ds(i * uc, uc)
            return rcopy(u_all.at[OWN, r], u_all.at[SIB, r], us_sib.at[i], ur_sib.at[i], sib)

        def u_cross(i):
            r = pl.ds(i * uc, uc)
            return rcopy(u_all.at[OWN, r], u_all.at[CROSS, r],
                         us_cross.at[i], ur_cross.at[i], cross)

        def u_fwd(i):
            r = pl.ds(i * uc, uc)
            return rcopy(u_all.at[CROSS, r], u_all.at[DIAG, r],
                         us_fwd.at[i], ur_diag.at[i], sib)

        def relay(i):
            u_cross(i).wait_recv()
            u_fwd(i).start()

        def norm_in(k, _):
            r = pl.ds(pl.multiple_of(k * 16, 16), 16)
            x = h0v[r, :].astype(F32)
            n = x * lax.rsqrt(jnp.mean(x * x, axis=-1, keepdims=True) + EPS)
            u_all[OWN, r, :] = (n * ln_ref[2:3, :]).astype(BF16)
            x1v[r, :] = (n * ln_ref[0:1, :]).astype(BF16)
            return 0

        lax.fori_loop(0, t // 32, norm_in, 0)
        pl.semaphore_wait(bar, 3)
        for i in range(UC // 2):
            u_cross(i).start()
            u_sib(i).start()
        lax.fori_loop(t // 32, t // 16, norm_in, 0)

        lg = lax.dot_general(wr_ref[...], u_all[OWN], (((1,), (1,)), ((), ())), preferred_element_type=F32)
        ex = lax.broadcasted_iota(jnp.int32, lg.shape, 0)
        lj = [jnp.sum(jnp.where(ex == idx_ref[j], lg, 0.0), axis=0, keepdims=True) for j in range(top)]
        mx = lj[0]
        for j in range(1, top):
            mx = jnp.maximum(mx, lj[j])
        ej = [jnp.exp(v - mx) for v in lj]
        tot = ej[0]
        for j in range(1, top):
            tot = tot + ej[j]
        mrow[OWN] = jnp.zeros((16, t), F32)
        for j in range(top):
            mrow[OWN, j:j + 1, :] = (idx_ref[j] * cap + slot_ref[j]).astype(F32)
            mrow[OWN, 8 + j:9 + j, :] = ej[j] / tot
        m_copies = [rcopy(mrow.at[OWN], mrow.at[role], ms.at[role - 1], mr.at[role - 1], dev)
                    for role, dev in ((SIB, sib), (CROSS, cross), (DIAG, diag))]
        for c in m_copies:
            c.start()
        for i in range(UC // 2, UC):
            u_cross(i).start()
            u_sib(i).start()

        def qkv(k, rope):
            a_dense(k).wait()

            for n in range(2):
                y = _dot(x1v[...], ring_a[k % NA, :, n * 512:(n + 1) * 512])
                for h in range(4):
                    yh = y[:, h * HEAD:(h + 1) * HEAD]
                    if rope:
                        yh = yh * cos_ref[...] + pltpu.roll(yh, HEAD // 2, 1) * sin_ref[...]
                    col = (k % 2) * (d // 2) + n * 512 + h * HEAD
                    xy[(k // 2) * t:(k // 2 + 1) * t, col:col + HEAD] = yh.astype(BF16)

        for k in range(6):
            qkv(k, k < 4)
            if k < 4:
                a_dense(k + NA).start()
            else:
                a_expert(0, k % NA - 0).start()
        for i in range(2):
            relay(i)
        for i in range(NB):
            b_ue2(i).start()

        ri = lax.broadcasted_iota(jnp.int32, (t, t), 0)
        ci = lax.broadcasted_iota(jnp.int32, (t, t), 1)

        def head_pair(hp, _):
            for s in range(2):
                col = pl.ds(pl.multiple_of((hp * 2 + s) * HEAD, HEAD), HEAD)
                q = xy[0:t, col]
                kk = xy[t:2 * t, col]
                vv = xy[2 * t:3 * t, col]
                sc = lax.dot_general(q, kk, (((1,), (1,)), ((), ())), preferred_element_type=F32) * HEAD ** -0.5
                sc = jnp.where(ri >= ci, sc, -1e30)
                p = jnp.exp(sc - jnp.max(sc, axis=-1, keepdims=True))
                p = (p / jnp.sum(p, axis=-1, keepdims=True)).astype(BF16)
                xy[0:t, col] = _dot(p, vv).astype(BF16)
            return 0

        lax.fori_loop(0, nh // 2, head_pair, 0)
        for i in range(2, 5):
            relay(i)

        for k in (6, 7):
            a_dense(k).wait()

            for n in range(2):
                col = slice((k % 2) * (d // 2) + n * 512, (k % 2) * (d // 2) + (n + 1) * 512)
                y = _dot(xy[0:t, :], ring_a[k % NA, :, n * 512:(n + 1) * 512])
                h0v[:, col] = (h0v[:, col].astype(F32) + y).astype(BF16)
            a_expert(1, k % NA).start()

        def norm_a(k, _):
            r = pl.ds(pl.multiple_of(k * 16, 16), 16)
            x = h0v[r, :].astype(F32)
            n = x * lax.rsqrt(jnp.mean(x * x, axis=-1, keepdims=True) + EPS)
            x1v[r, :] = (n * ln_ref[1:2, :]).astype(BF16)
            return 0

        lax.fori_loop(0, t // 16, norm_a, 0)

        for c in m_copies:
            c.wait()
        for role in range(4):
            mcol[role] = jnp.transpose(jnp.concatenate([mrow[role], jnp.zeros((112, t), F32)], axis=0))
        for i in range(5, UC):
            relay(i)
        for i in range(UC):
            u_sib(i).wait()
            u_cross(i).wait_send()
            u_fwd(i).wait()

        def swiglu(src, sr, sl, dst, dr):
            for n0 in range(0, fe - fe % 256, 256):
                cols = slice(n0, n0 + 256)
                y1 = _dot(src[sr, :], ring_a[sl, :, cols])
                y3 = _dot(src[sr, :], ring_a[sl + 1, :, cols])
                dst[dr, cols] = (y1 * jax.nn.sigmoid(y1) * y3).astype(BF16)
            if fe % 256:
                cols = slice(fe - fe % 256, fe)
                y = _dot(src[sr, :], jnp.concatenate([ring_a[sl, :, cols], ring_a[sl + 1, :, cols]], axis=1))
                y1, y3 = y[:, :fe % 256], y[:, fe % 256:]
                dst[dr, cols] = (y1 * jax.nn.sigmoid(y1) * y3).astype(BF16)

        npart = 4 * t // el
        def gate_part(i):
            role = lax.div(i, el // 4)
            r = pl.ds(pl.multiple_of(lax.rem(i, el // 4) * npart, npart), npart)
            for b in range(rl // 256):
                rr = (lax.broadcasted_iota(jnp.int32, (npart, 256), 1) + b * 256).astype(F32) + base
                w = jnp.zeros((npart, 256), F32)
                for j in range(top):
                    w = jnp.where(rr == mcol[role, r, j:j + 1], mcol[role, r, 8 + j:9 + j], w)
                for part in range(3):
                    piece = w.astype(BF16)
                    comb[role, r, part * rl + b * 256:part * rl + (b + 1) * 256] = piece
                    w = w - piece.astype(F32)

        def group(g, _):
            def gather(role, _):
                rr = (lax.broadcasted_iota(jnp.int32, (rows, t), 0) + g * rows).astype(F32) + base
                hit = rr == mrow[role, 0:1, :]
                for j in range(1, top):
                    hit = hit | (rr == mrow[role, j:j + 1, :])
                oh = jnp.where(hit, 1.0, 0.0).astype(BF16)
                for n in range(d // 512):
                    xg = _dot(oh, u_all[role, :, n * 512:(n + 1) * 512]).astype(BF16)
                    for e4 in range(4):
                        xy[pl.ds(pl.multiple_of(e4 * rows + role * cap, 16), cap), n * 512:(n + 1) * 512] = (
                            xg[e4 * cap:(e4 + 1) * cap, :])
                return 0

            lax.fori_loop(0, 4, gather, 0)

            def pair(pp, _):
                e0 = g * 4 + pp * 2
                for s in range(2):
                    e = e0 + s
                    xr = pl.ds(pl.multiple_of((pp * 2 + s) * rows, 16), rows)
                    hr = pl.ds(pl.multiple_of(e * rows, 16), rows)
                    gate_part(e)
                    a_expert(e, 2 * s).wait()
                    a_expert(e, 2 * s + 1).wait()
                    swiglu(xy, xr, 2 * s, he, hr)

                    @pl.when(e0 + 2 < el)
                    def _():
                        a_expert(e + 2, 2 * s).start()
                        a_expert(e + 2, 2 * s + 1).start()

                    @pl.when(e0 + 2 >= el)
                    def _():
                        a_shared(2 * s).start()
                        a_shared(2 * s + 1).start()
                return 0

            lax.fori_loop(0, 2, pair, 0)
            return 0

        lax.fori_loop(0, el // 4, group, 0)

        def c_diag(c):
            return rcopy(sdiag.at[lax.rem(c, 2)], rdiag.at[c], cs_diag.at[c], cr_diag.at[c], sib)

        def c_sib(c):
            return rcopy(ssib.at[lax.rem(c, 2)], rsib.at[lax.rem(c, 2)], cs_sib.at[c], cr_sib.at[c], sib)

        def c_cross(c):
            return rcopy(rdiag.at[c], rcross.at[c], cs_cross.at[c], cr_cross.at[c], cross)

        def partial(role):
            yc = xy[:, role * CC:(role + 1) * CC]
            return (_dot(comb[role, :, 0:rl], yc) + _dot(comb[role, :, rl:2 * rl], yc)
                    + _dot(comb[role, :, 2 * rl:3 * rl], yc))

        def chunk(c, _):
            def four(q, _):
                i = c * (el // EB) + q
                sl = lax.rem(i, NB)
                b_ue2(i).wait()
                for s in range(EB):
                    e = q * EB + s
                    y = _dot(he[pl.ds(pl.multiple_of(e * rows, 16), rows), :], ring_b[sl, s]).astype(BF16)
                    for role in range(4):
                        xy[pl.ds(pl.multiple_of(e * cap, 16), cap), role * CC:(role + 1) * CC] = (
                            y[role * cap:(role + 1) * cap, :])

                @pl.when(i + NB < nue2)
                def _():
                    b_ue2(i + NB).start()

                @pl.when(i + NB >= nue2)
                def _():
                    for cp in b_ws2(i + NB):
                        cp.start()
                return 0

            lax.fori_loop(0, el // EB, four, 0)

            @pl.when(c >= 2)
            def _():
                c_diag(c - 2).wait_send()
                c_sib(c - 2).wait_send()

            sdiag[lax.rem(c, 2)] = partial(DIAG)
            c_diag(c).start()
            ssib[lax.rem(c, 2)] = partial(SIB)
            c_sib(c).start()
            macc[c] = partial(OWN)
            pc = partial(CROSS)
            c_diag(c).wait_recv()
            rdiag[c] = rdiag[c] + pc
            c_cross(c).start()
            c_sib(c).wait_recv()
            macc[c] = macc[c] + rsib[lax.rem(c, 2)]
            return 0

        lax.fori_loop(0, nch, chunk, 0)

        for half in range(nf):
            a_shared(2 * half).wait()
            a_shared(2 * half + 1).wait()
            swiglu(x1v, slice(0, t), 2 * half, he, slice(half * t, (half + 1) * t))

        def shared_out(k, _):
            i = k + nue2
            for cp in b_ws2(i):
                cp.wait()
            for u in range(cpt):
                f = macc[k * cpt + u]
                for half in range(nf):
                    f = f + _dot(he[half * t:(half + 1) * t, :], ring_b[lax.rem(i, NB), u * nf + half])
                macc[k * cpt + u] = f

            @pl.when(k + NB < nws2)
            def _():
                for cp in b_ws2(i + NB):
                    cp.start()
            return 0

        lax.fori_loop(0, nws2, shared_out, 0)
        for c in range(nch):
            cols = slice(c * CC, (c + 1) * CC)
            c_cross(c).wait_recv()

            def fin(k, _):
                r = pl.ds(pl.multiple_of(k * 32, 32), 32)
                x1v[r, cols] = (h0v[r, cols].astype(F32) + macc[c, r] + rcross[c, r]).astype(BF16)
                return 0

            lax.fori_loop(0, t // 32, fin, 0)
            pltpu.make_async_copy(x1v.at[:, pl.ds(c * CC, CC)], out_hbm.at[:, pl.ds(c * CC, CC)],
                                  sem_out.at[c]).start()
        for c in range(nch):
            if c >= nch - 2:
                c_diag(c).wait_send()
                c_sib(c).wait_send()
            c_cross(c).wait_send()
            pltpu.make_async_copy(x1v.at[:, pl.ds(c * CC, CC)], out_hbm.at[:, pl.ds(c * CC, CC)],
                                  sem_out.at[c]).wait()

    dma = pltpu.SemaphoreType.DMA
    vm = pltpu.VMEM
    any_ = pl.BlockSpec(memory_space=pl.ANY)
    vmem = pl.BlockSpec(memory_space=pltpu.VMEM)
    return pl.pallas_call(
        kernel,
        out_shape=jax.ShapeDtypeStruct((t, d), BF16),
        in_specs=[any_] + [vmem] * 8 + [any_] * 10,
        out_specs=any_,
        scratch_shapes=[
            vm((NA, d, fe), BF16),
            vm((NB, EB, fe, CC), BF16),
            vm((4, t, d), BF16),
            vm((4, t, 3 * rl), BF16),
            vm((max(4 * rows, 3 * t, rl), d), BF16),
            vm((el * rows, fe), BF16),
            vm((8, d), F32),
            vm((t, d), BF16),
            vm((t, d), BF16),
            vm((4, 16, t), F32),
            vm((4, t, 128), F32),
            vm((nch, t, CC), F32),
            vm((2, t, CC), F32),
            vm((nch, t, CC), F32),
            vm((nch, t, CC), F32),
            vm((2, t, CC), F32),
            vm((2, t, CC), F32),
            dma((NA,)), dma((NB, EB)), dma, dma((nch,)),
            dma((3,)), dma((3,)),
            dma((UC,)), dma((UC,)), dma((UC,)), dma((UC,)), dma((UC,)), dma((UC,)),
            dma((nch,)), dma((nch,)), dma((nch,)), dma((nch,)), dma((nch,)), dma((nch,)),
        ],
        compiler_params=pltpu.CompilerParams(collective_id=0, has_side_effects=True,
                                             vmem_limit_bytes=67043328),
        name='moe_layer',
    )


def solution(mesh):
    g_ = mesh.shape['ep']
    rows = P(('dp', 'ep'))
    rep = P()

    def local(h0, idx, slot, ln_attn, wq, wk, wv, wo, ln_ffn, ws1, ws3, ws2, ln_moe, wr, ue1, ue3, ue2):
        b, s, d = h0.shape
        top = idx.shape[-1]
        el, _, fe = ue1.shape
        t = b * s
        cap = CAP_FACTOR * t * top // (el * g_)
        cos, sin = _rope_tables(s)
        gains = [w.reshape(d // 128, 128) for w in (ln_attn, ln_ffn, ln_moe)]
        ids = [jnp.transpose(a, (2, 0, 1)).reshape(top, 1, t) for a in (idx, slot)]
        call = _build(t, d, fe, ws1.shape[1], el, cap, top)
        out = call(h0.reshape(t, d), *ids, *gains, cos, sin, wr.T,
                   wq, wk, wv, wo, ws1, ws3, ws2, ue1, ue3, ue2)
        return out.reshape(b, s, d)

    specs = (rows, rows, rows) + (rep,) * 11 + (P('ep'), P('ep'), P('ep'))
    return jax.shard_map(local, mesh=mesh, in_specs=specs, out_specs=rows, check_vma=False)
```

```python
import jax
import jax.numpy as jnp
import numpy as np
from jax import lax
from jax.experimental import pallas as pl
from jax.experimental.pallas import tpu as pltpu
from jax.sharding import PartitionSpec as P

MESH = pl.DeviceIdType.MESH
F32 = jnp.float32
BF16 = jnp.bfloat16
EPS = 1e-6
HEAD = 128
CAP_FACTOR = 2

OWN, SIB, CROSS, DIAG = range(4)
NA = 4
NB = 4
EB = 4
ND = 4
CC = 256
UC = 4


def _dot(a, b):
    return jnp.dot(a, b, preferred_element_type=F32)


def _rope_tables(s):
    half = HEAD // 2
    freq = np.float32(10000.0) ** (-np.arange(half, dtype=np.float32) / np.float32(half))
    ang = np.arange(s, dtype=np.float32)[:, None] * freq.astype(np.float32)[None, :]
    c, sn = np.cos(ang), np.sin(ang)
    return np.concatenate([c, c], 1).astype(np.float32), np.concatenate([-sn, sn], 1).astype(np.float32)


def _build(t, d, fe, fs, el, cap, top):
    nh = d // HEAD
    rows = 4 * cap
    rl = el * cap
    nch = d // CC
    uc = t // UC
    nta = 8 + 2 * el
    nue2 = nch * el // EB
    nf = fs // fe
    cpt = EB // nf
    nws2 = nch // cpt
    assert el == NB * EB and nws2 == NB

    def kernel(h0_hbm, idx_ref, slot_ref, lna_ref, lnf_ref, lnm_ref, cos_ref, sin_ref, wr_ref, wq, wk, wv, wo, ws1, ws3, ws2,
               ue1, ue3, ue2, out_hbm,
               ring_a, ring_b, u_all, comb, xy, he, ln_ref, h0v, x1v, mrow,
               macc, rsib, rcross, rdiag, sdiag, ssib,
               sem_a, sem_b, sem_in, sem_out,
               ms, mr, us_sib, ur_sib, us_cross, ur_cross, us_fwd, ur_diag,
               cs_diag, cr_diag, cs_sib, cr_sib, cs_cross, cr_cross):
        me = lax.axis_index('ep')
        core = lax.rem(me, 2)
        sib = me + 1 - 2 * core
        cross = lax.rem(me + 2, 4)
        diag = lax.rem(sib + 2, 4)
        base = (me * rl).astype(F32)

        def rcopy(src, dst, ssem, rsem, dev):
            return pltpu.make_async_remote_copy(src_ref=src, dst_ref=dst, send_sem=ssem, recv_sem=rsem,
                                                device_id={'ep': dev}, device_id_type=MESH)

        def a_dense(k):
            w = (wq, wk, wv, wo)[k // 2]
            return pltpu.make_async_copy(w.at[:, pl.ds((k % 2) * (d // 2), d // 2)],
                                         ring_a.at[k % NA, :, pl.ds(0, d // 2)], sem_a.at[k % NA])

        def a_expert(e, s):
            return pltpu.make_async_copy((ue1, ue3)[s % 2].at[e], ring_a.at[s], sem_a.at[s])

        def a_shared(k):
            return pltpu.make_async_copy((ws1, ws3)[k % 2].at[:, pl.ds((k // 2) * fe, fe)],
                                         ring_a.at[k], sem_a.at[k])

        def b_ue2(i, sl):
            e0 = lax.rem(i, el // EB) * EB
            col = pl.multiple_of(lax.div(i, el // EB) * CC, CC)
            return pltpu.make_async_copy(ue2.at[pl.ds(e0, EB), :, pl.ds(col, CC)], ring_b.at[sl], sem_b.at[sl, 0])

        def b_ws2(i, sl):
            k = i - nue2
            return [pltpu.make_async_copy(
                ws2.at[pl.ds(half * fe, fe), pl.ds(pl.multiple_of((k * cpt + u) * CC, CC), CC)],
                ring_b.at[sl, u * nf + half], sem_b.at[sl, u * nf + half])
                for u in range(cpt) for half in range(nf)]

        h0_in = pltpu.make_async_copy(h0_hbm, h0v, sem_in)
        h0_in.start()
        bar = pltpu.get_barrier_semaphore()
        for dev in (sib, cross, diag):
            pl.semaphore_signal(bar, inc=1, device_id={'ep': dev}, device_id_type=MESH)
        for k, ref in enumerate((lna_ref, lnf_ref, lnm_ref)):
            w = ref[...].astype(F32)
            for i in range(d // 128):
                ln_ref[k:k + 1, i * 128:(i + 1) * 128] = w[i:i + 1, :]
        h0_in.wait()
        for k in range(NA):
            a_dense(k).start()

        def u_sib(i):
            r = pl.ds(i * uc, uc)
            return rcopy(u_all.at[OWN, r], u_all.at[SIB, r], us_sib.at[i], ur_sib.at[i], sib)

        def u_cross(i):
            r = pl.ds(i * uc, uc)
            return rcopy(u_all.at[OWN, r], u_all.at[CROSS, r],
                         us_cross.at[i], ur_cross.at[i], cross)

        def u_fwd(i):
            r = pl.ds(i * uc, uc)
            return rcopy(u_all.at[CROSS, r], u_all.at[DIAG, r],
                         us_fwd.at[i], ur_diag.at[i], sib)

        def relay(i):
            u_cross(i).wait_recv()
            u_fwd(i).start()

        def norm_in(k, _):
            r = pl.ds(pl.multiple_of(k * 16, 16), 16)
            x = h0v[r, :].astype(F32)
            n = x * lax.rsqrt(jnp.mean(x * x, axis=-1, keepdims=True) + EPS)
            u_all[OWN, r, :] = (n * ln_ref[2:3, :]).astype(BF16)
            x1v[r, :] = (n * ln_ref[0:1, :]).astype(BF16)
            return 0

        lax.fori_loop(0, t // 32, norm_in, 0)
        pl.semaphore_wait(bar, 3)
        for i in range(UC // 2):
            u_cross(i).start()
            u_sib(i).start()
        lax.fori_loop(t // 32, t // 16, norm_in, 0)

        lg = lax.dot_general(wr_ref[...], u_all[OWN], (((1,), (1,)), ((), ())), preferred_element_type=F32)
        ex = lax.broadcasted_iota(jnp.int32, lg.shape, 0)
        lj = [jnp.sum(jnp.where(ex == idx_ref[j], lg, 0.0), axis=0, keepdims=True) for j in range(top)]
        mx = lj[0]
        for j in range(1, top):
            mx = jnp.maximum(mx, lj[j])
        ej = [jnp.exp(v - mx) for v in lj]
        tot = ej[0]
        for j in range(1, top):
            tot = tot + ej[j]
        mrow[OWN] = jnp.zeros((16, t), F32)
        for j in range(top):
            mrow[OWN, j:j + 1, :] = (idx_ref[j] * cap + slot_ref[j]).astype(F32)
            mrow[OWN, 8 + j:9 + j, :] = ej[j] / tot
        m_copies = [rcopy(mrow.at[OWN], mrow.at[role], ms.at[role - 1], mr.at[role - 1], dev)
                    for role, dev in ((SIB, sib), (CROSS, cross), (DIAG, diag))]
        for c in m_copies:
            c.start()
        for i in range(UC // 2, UC):
            u_cross(i).start()
            u_sib(i).start()

        def qkv(k, rope):
            a_dense(k).wait()

            for n in range(2):
                y = _dot(x1v[...], ring_a[k % NA, :, n * 512:(n + 1) * 512])
                for h in range(4):
                    yh = y[:, h * HEAD:(h + 1) * HEAD]
                    if rope:
                        yh = yh * cos_ref[...] + pltpu.roll(yh, HEAD // 2, 1) * sin_ref[...]
                    col = (k % 2) * (d // 2) + n * 512 + h * HEAD
                    xy[(k // 2) * t:(k // 2 + 1) * t, col:col + HEAD] = yh.astype(BF16)

        for k in range(6):
            qkv(k, k < 4)
            if k < 4:
                a_dense(k + NA).start()
            else:
                a_expert(0, k % NA - 0).start()
        relay(0)
        for i in range(NB):
            b_ue2(i, i).start()

        ri = lax.broadcasted_iota(jnp.int32, (t, t), 0)
        ci = lax.broadcasted_iota(jnp.int32, (t, t), 1)

        def head_pair(hp, _):
            for s in range(2):
                col = pl.ds(pl.multiple_of((hp * 2 + s) * HEAD, HEAD), HEAD)
                q = xy[0:t, col]
                kk = xy[t:2 * t, col]
                vv = xy[2 * t:3 * t, col]
                sc = lax.dot_general(q, kk, (((1,), (1,)), ((), ())), preferred_element_type=F32) * HEAD ** -0.5
                sc = jnp.where(ri >= ci, sc, -1e30)
                p = jnp.exp(sc - jnp.max(sc, axis=-1, keepdims=True))
                p = (p / jnp.sum(p, axis=-1, keepdims=True)).astype(BF16)
                xy[0:t, col] = _dot(p, vv).astype(BF16)
            return 0

        lax.fori_loop(0, nh // 2, head_pair, 0)
        relay(1)

        for k in (6, 7):
            a_dense(k).wait()

            for n in range(2):
                col = slice((k % 2) * (d // 2) + n * 512, (k % 2) * (d // 2) + (n + 1) * 512)
                y = _dot(xy[0:t, :], ring_a[k % NA, :, n * 512:(n + 1) * 512])
                h0v[:, col] = (h0v[:, col].astype(F32) + y).astype(BF16)
            a_expert(1, k % NA).start()

        def norm_a(k, _):
            r = pl.ds(pl.multiple_of(k * 16, 16), 16)
            x = h0v[r, :].astype(F32)
            n = x * lax.rsqrt(jnp.mean(x * x, axis=-1, keepdims=True) + EPS)
            x1v[r, :] = (n * ln_ref[1:2, :]).astype(BF16)
            return 0

        lax.fori_loop(0, t // 16, norm_a, 0)

        for c in m_copies:
            c.wait()
        for role in range(4):
            macc[role, :, 0:128] = jnp.transpose(jnp.concatenate([mrow[role], jnp.zeros((112, t), F32)], axis=0))
        for i in range(2, UC):
            relay(i)
        for i in range(UC):
            u_sib(i).wait()
            u_cross(i).wait_send()
            u_fwd(i).wait()

        def swiglu(src, sr, sl, dst, dr, between=()):
            between = list(between)
            for n0 in range(0, fe - fe % 256, 256):
                cols = slice(n0, n0 + 256)
                y1 = _dot(src[sr, :], ring_a[sl, :, cols])
                y3 = _dot(src[sr, :], ring_a[sl + 1, :, cols])
                dst[dr, cols] = (y1 * jax.nn.sigmoid(y1) * y3).astype(BF16)
                if between:
                    between.pop(0)()
            if fe % 256:
                cols = slice(fe - fe % 256, fe)
                y = _dot(src[sr, :], jnp.concatenate([ring_a[sl, :, cols], ring_a[sl + 1, :, cols]], axis=1))
                y1, y3 = y[:, :fe % 256], y[:, fe % 256:]
                dst[dr, cols] = (y1 * jax.nn.sigmoid(y1) * y3).astype(BF16)

        def gather(e, buf, role):
            rr = (lax.broadcasted_iota(jnp.int32, (cap, t), 0) + e * cap).astype(F32) + base
            hit = rr == mrow[role, 0:1, :]
            for j in range(1, top):
                hit = hit | (rr == mrow[role, j:j + 1, :])
            oh = jnp.where(hit, 1.0, 0.0).astype(BF16)
            r0 = buf * rows + role * cap
            for n in range(d // 512):
                xy[r0:r0 + cap, n * 512:(n + 1) * 512] = _dot(oh, u_all[role, :, n * 512:(n + 1) * 512]).astype(BF16)

        npart = 4 * t // el
        def gate_part(i):
            role = lax.div(i, el // 4)
            r = pl.ds(pl.multiple_of(lax.rem(i, el // 4) * npart, npart), npart)
            for b in range(rl // 256):
                rr = (lax.broadcasted_iota(jnp.int32, (npart, 256), 1) + b * 256).astype(F32) + base
                w = jnp.zeros((npart, 256), F32)
                for j in range(top):
                    w = jnp.where(rr == macc[role, r, j:j + 1], macc[role, r, 8 + j:9 + j], w)
                for part in range(3):
                    piece = w.astype(BF16)
                    comb[role, r, part * rl + b * 256:part * rl + (b + 1) * 256] = piece
                    w = w - piece.astype(F32)

        for role in range(4):
            gather(0, 0, role)

        def pair(p, _):
            for s in range(2):
                e = p * 2 + s
                a_expert(e, 2 * s).wait()
                a_expert(e, 2 * s + 1).wait()
                gate_part(e)
                swiglu(xy, slice(s * rows, (s + 1) * rows), 2 * s,
                       he, pl.ds(pl.multiple_of(e * rows, 16), rows),
                       [lambda role=role: gather(e + 1, 1 - s, role) for role in range(4)])

                @pl.when(e + 2 < el)
                def _():
                    a_expert(e + 2, 2 * s).start()
                    a_expert(e + 2, 2 * s + 1).start()
            return 0

        lax.fori_loop(0, el // 2, pair, 0)

        def c_diag(c):
            return rcopy(sdiag.at[lax.rem(c, 2)], rdiag.at[lax.rem(c, ND)], cs_diag.at[c], cr_diag.at[c], sib)

        def c_sib(c):
            return rcopy(ssib.at[lax.rem(c, 2)], rsib.at[lax.rem(c, 2)], cs_sib.at[c], cr_sib.at[c], sib)

        def c_cross(c):
            return rcopy(rdiag.at[lax.rem(c, ND)], rcross.at[c], cs_cross.at[c], cr_cross.at[c], cross)

        def partial(role):
            yc = xy[:, role * CC:(role + 1) * CC]
            return _dot(comb[role], jnp.concatenate([yc, yc, yc], axis=0))

        def add_sib(c):
            c_sib(c).wait_recv()
            macc[c] = macc[c] + rsib[lax.rem(c, 2)]

        def chunk(c, _):
            @pl.when(c >= 1)
            def _():
                add_sib(c - 1)

            @pl.when(c >= 2)
            def _():
                c_diag(c - 2).wait_send()
                c_sib(c - 2).wait_send()

            @pl.when(c >= ND - 1)
            def _():
                c_cross(c - (ND - 1)).wait_send()

            @pl.when((c >= 1) & (c <= 2 * nf))
            def _():
                for k in range(2 * nf):
                    @pl.when(c == k + 1)
                    def _():
                        a_shared(k).start()

            for blk in range(2):
                slots = range(blk * (NB // 2), (blk + 1) * (NB // 2))
                for sl in slots:
                    b_ue2(c * NB + sl, sl).wait()
                for sl in slots:
                    for s in range(EB):
                        e = sl * EB + s
                        y = _dot(he[e * rows:(e + 1) * rows, :], ring_b[sl, s]).astype(BF16)
                        for role in range(4):
                            xy[e * cap:(e + 1) * cap, role * CC:(role + 1) * CC] = y[role * cap:(role + 1) * cap, :]

                @pl.when(c + 1 < nch)
                def _():
                    for sl in slots:
                        b_ue2((c + 1) * NB + sl, sl).start()

                @pl.when(c + 1 == nch)
                def _():
                    for sl in slots:
                        for cp in b_ws2(nue2 + sl, sl):
                            cp.start()

            sdiag[lax.rem(c, 2)] = partial(DIAG)
            ssib[lax.rem(c, 2)] = partial(SIB)
            c_diag(c).start()
            c_sib(c).start()
            pc = partial(CROSS)
            macc[c] = partial(OWN)
            c_diag(c).wait_recv()
            rdiag[lax.rem(c, ND)] = rdiag[lax.rem(c, ND)] + pc
            c_cross(c).start()
            return 0

        lax.fori_loop(0, nch, chunk, 0)
        add_sib(nch - 1)

        for half in range(nf):
            a_shared(2 * half).wait()
            a_shared(2 * half + 1).wait()
            swiglu(x1v, slice(0, t), 2 * half, he, slice(half * t, (half + 1) * t))

        for k in range(nws2):
            for cp in b_ws2(nue2 + k, k):
                cp.wait()

        def shared_out(k, _):
            for u in range(cpt):
                f = macc[k * cpt + u]
                for half in range(nf):
                    f = f + _dot(he[half * t:(half + 1) * t, :], ring_b[k, u * nf + half])
                macc[k * cpt + u] = f
            return 0

        lax.fori_loop(0, nws2, shared_out, 0)
        for c in range(nch):
            cols = slice(c * CC, (c + 1) * CC)
            c_cross(c).wait_recv()

            def fin(k, _):
                r = pl.ds(pl.multiple_of(k * 32, 32), 32)
                x1v[r, cols] = (h0v[r, cols].astype(F32) + macc[c, r] + rcross[c, r]).astype(BF16)
                return 0

            lax.fori_loop(0, t // 32, fin, 0)
            pltpu.make_async_copy(x1v.at[:, pl.ds(c * CC, CC)], out_hbm.at[:, pl.ds(c * CC, CC)],
                                  sem_out.at[c]).start()
        for c in range(nch):
            if c >= nch - 2:
                c_diag(c).wait_send()
                c_sib(c).wait_send()
            if c >= nch - (ND - 1):
                c_cross(c).wait_send()
            pltpu.make_async_copy(x1v.at[:, pl.ds(c * CC, CC)], out_hbm.at[:, pl.ds(c * CC, CC)],
                                  sem_out.at[c]).wait()

    dma = pltpu.SemaphoreType.DMA
    vm = pltpu.VMEM
    any_ = pl.BlockSpec(memory_space=pl.ANY)
    vmem = pl.BlockSpec(memory_space=pltpu.VMEM)
    return pl.pallas_call(
        kernel,
        out_shape=jax.ShapeDtypeStruct((t, d), BF16),
        in_specs=[any_] + [vmem] * 8 + [any_] * 10,
        out_specs=any_,
        scratch_shapes=[
            vm((NA, d, fe), BF16),
            vm((NB, EB, fe, CC), BF16),
            vm((4, t, d), BF16),
            vm((4, t, 3 * rl), BF16),
            vm((max(4 * rows, 3 * t, rl), d), BF16),
            vm((el * rows, fe), BF16),
            vm((8, d), F32),
            vm((t, d), BF16),
            vm((t, d), BF16),
            vm((4, 16, t), F32),
            vm((nch, t, CC), F32),
            vm((2, t, CC), F32),
            vm((nch, t, CC), F32),
            vm((ND, t, CC), F32),
            vm((2, t, CC), F32),
            vm((2, t, CC), F32),
            dma((NA,)), dma((NB, EB)), dma, dma((nch,)),
            dma((3,)), dma((3,)),
            dma((UC,)), dma((UC,)), dma((UC,)), dma((UC,)), dma((UC,)), dma((UC,)),
            dma((nch,)), dma((nch,)), dma((nch,)), dma((nch,)), dma((nch,)), dma((nch,)),
        ],
        compiler_params=pltpu.CompilerParams(collective_id=0, has_side_effects=True,
                                             vmem_limit_bytes=67043328),
        name='moe_layer',
    )


def solution(mesh):
    g_ = mesh.shape['ep']
    rows = P(('dp', 'ep'))
    rep = P()

    def local(h0, idx, slot, ln_attn, wq, wk, wv, wo, ln_ffn, ws1, ws3, ws2, ln_moe, wr, ue1, ue3, ue2):
        b, s, d = h0.shape
        top = idx.shape[-1]
        el, _, fe = ue1.shape
        t = b * s
        cap = CAP_FACTOR * t * top // (el * g_)
        cos, sin = _rope_tables(s)
        gains = [w.reshape(d // 128, 128) for w in (ln_attn, ln_ffn, ln_moe)]
        ids = [jnp.transpose(a, (2, 0, 1)).reshape(top, 1, t) for a in (idx, slot)]
        call = _build(t, d, fe, ws1.shape[1], el, cap, top)
        out = call(h0.reshape(t, d), *ids, *gains, cos, sin, wr.T,
                   wq, wk, wv, wo, ws1, ws3, ws2, ue1, ue3, ue2)
        return out.reshape(b, s, d)

    specs = (rows, rows, rows) + (rep,) * 11 + (P('ep'), P('ep'), P('ep'))
    return jax.shard_map(local, mesh=mesh, in_specs=specs, out_specs=rows, check_vma=False)
```

```python
import jax
import jax.numpy as jnp
import numpy as np
from jax import lax
from jax.experimental import pallas as pl
from jax.experimental.pallas import tpu as pltpu
from jax.sharding import PartitionSpec as P

MESH = pl.DeviceIdType.MESH
F32 = jnp.float32
BF16 = jnp.bfloat16
EPS = 1e-6
HEAD = 128
CAP_FACTOR = 2

OWN, SIB, CROSS, DIAG = range(4)
NA = 4
NB = 4
EB = 4
CC = 256
UC = 4


def _dot(a, b):
    return jnp.dot(a, b, preferred_element_type=F32)


def _rope_tables(s):
    half = HEAD // 2
    freq = np.float32(10000.0) ** (-np.arange(half, dtype=np.float32) / np.float32(half))
    ang = np.arange(s, dtype=np.float32)[:, None] * freq.astype(np.float32)[None, :]
    c, sn = np.cos(ang), np.sin(ang)
    return np.concatenate([c, c], 1).astype(np.float32), np.concatenate([-sn, sn], 1).astype(np.float32)


def _build(t, d, fe, fs, el, cap, top):
    nh = d // HEAD
    rows = 4 * cap
    rl = el * cap
    nch = d // CC
    uc = t // UC
    nta = 8 + 2 * el
    nue2 = nch * el // EB
    dh = d // 2
    fh = fe // 2 // 256 * 256 + 256
    nf = fs // fe
    cpt = EB // nf
    nws2 = nch // cpt
    assert el == NB * EB and nws2 == NB

    def kernel(h0_hbm, idx_hbm, slot_hbm, lna_hbm, lnf_hbm, lnm_hbm, cos_hbm, sin_hbm, wr_hbm, wq, wk, wv, wo, ws1, ws3, ws2,
               ue1, ue3, ue2, out_hbm,
               idx_ref, slot_ref, gain_ref,
               ring_a, ring_b, u_all, comb, xbuf, ybuf, he, ln_ref, h0v, mrow,
               macc, rsib, rcross, rdiag, sdiag, ssib, pcs,
               sem_a, sem_b, sem_in, sem_small, sem_out,
               ms, mr, us_sib, ur_sib, us_cross, ur_cross, us_fwd, ur_diag,
               cs_diag, cr_diag, cs_sib, cr_sib, cs_cross, cr_cross):
        me = lax.axis_index('ep')
        core = lax.rem(me, 2)
        sib = me + 1 - 2 * core
        cross = lax.rem(me + 2, 4)
        diag = lax.rem(sib + 2, 4)
        base = (me * rl).astype(F32)

        def rcopy(src, dst, ssem, rsem, dev):
            return pltpu.make_async_remote_copy(src_ref=src, dst_ref=dst, send_sem=ssem, recv_sem=rsem,
                                                device_id={'ep': dev}, device_id_type=MESH)

        def a_dense(k):
            w = (wq, wk, wv, wo)[k // 2]
            return pltpu.make_async_copy(w.at[:, pl.ds((k % 2) * (d // 2), d // 2)],
                                         ring_a.at[k % NA, :, pl.ds(0, d // 2)], sem_a.at[k % NA, 0])

        def a_expert(e, s, h):
            cols = pl.ds(h * fh, (fh, fe - fh)[h])
            return pltpu.make_async_copy((ue1, ue3)[s % 2].at[e, :, cols], ring_a.at[s, :, cols], sem_a.at[s, h])

        def a_shared(k):
            return pltpu.make_async_copy((ws1, ws3)[k % 2].at[:, pl.ds((k // 2) * fe, fe)],
                                         ring_a.at[k], sem_a.at[k, 0])

        def b_ue2(i, sl):
            e0 = lax.rem(i, el // EB) * EB
            col = pl.multiple_of(lax.div(i, el // EB) * CC, CC)
            return pltpu.make_async_copy(ue2.at[pl.ds(e0, EB), :, pl.ds(col, CC)], ring_b.at[sl], sem_b.at[sl, 0])

        def b_ws2(i, sl):
            k = i - nue2
            return [pltpu.make_async_copy(
                ws2.at[pl.ds(half * fe, fe), pl.ds(pl.multiple_of((k * cpt + u) * CC, CC), CC)],
                ring_b.at[sl, u * nf + half], sem_b.at[sl, u * nf + half])
                for u in range(cpt) for half in range(nf)]

        h0_in = [pltpu.make_async_copy(h0_hbm.at[pl.ds(i * uc, uc)], h0v.at[pl.ds(i * uc, uc)], sem_in.at[i])
                 for i in range(UC)]
        small = [pltpu.make_async_copy(a, b, sem_small.at[i]) for i, (a, b) in enumerate((
            (lna_hbm, gain_ref.at[0]), (lnf_hbm, gain_ref.at[1]), (lnm_hbm, gain_ref.at[2]), (idx_hbm, idx_ref),
            (slot_hbm, slot_ref), (wr_hbm, xbuf.at[pl.ds(0, el * 4)]), (cos_hbm, macc.at[4, :, pl.ds(0, HEAD)]),
            (sin_hbm, macc.at[5, :, pl.ds(0, HEAD)])))]
        for cp in small[:3] + h0_in + small[3:]:
            cp.start()
        bar = pltpu.get_barrier_semaphore()
        for dev in (sib, cross, diag):
            pl.semaphore_signal(bar, inc=1, device_id={'ep': dev}, device_id_type=MESH)
        for k in range(3):
            small[k].wait()
        for k in range(3):
            w = gain_ref[k].astype(F32)
            for i in range(d // 128):
                ln_ref[k:k + 1, i * 128:(i + 1) * 128] = w[i:i + 1, :]

        def u_sib(i):
            r = pl.ds(i * uc, uc)
            return rcopy(u_all.at[OWN, r], u_all.at[SIB, r], us_sib.at[i], ur_sib.at[i], sib)

        def u_cross(i):
            r = pl.ds(i * uc, uc)
            return rcopy(u_all.at[OWN, r], u_all.at[CROSS, r],
                         us_cross.at[i], ur_cross.at[i], cross)

        def u_fwd(i):
            r = pl.ds(i * uc, uc)
            return rcopy(u_all.at[CROSS, r], u_all.at[DIAG, r],
                         us_fwd.at[i], ur_diag.at[i], sib)

        def relay(i):
            u_cross(i).wait_recv()
            u_fwd(i).start()

        def norm_in(k, _):
            r = pl.ds(pl.multiple_of(k * 16, 16), 16)
            x = h0v[r, :].astype(F32)
            n = x * lax.rsqrt(jnp.mean(x * x, axis=-1, keepdims=True) + EPS)
            u_all[OWN, r, :] = (n * ln_ref[2:3, :]).astype(BF16)
            x1 = (n * ln_ref[0:1, :]).astype(BF16)
            for half in range(2):
                he[pl.ds(pl.multiple_of((6 + half) * t + k * 16, 16), 16), 0:dh] = x1[:, half * dh:(half + 1) * dh]
            return 0

        def halves(k):
            return jnp.concatenate([he[k * t:(k + 1) * t, 0:dh], he[(k + 1) * t:(k + 2) * t, 0:dh]], axis=1)

        for i in range(UC):
            h0_in[i].wait()
            if i == 1:
                for k in range(NA):
                    a_dense(k).start()
            lax.fori_loop(i * uc // 16, (i + 1) * uc // 16, norm_in, 0)
            if i == 0:
                pl.semaphore_wait(bar, 3)
            if i < UC // 2:
                u_cross(i).start()
                u_sib(i).start()
        for k in range(3, 8):
            small[k].wait()

        lg = lax.dot_general(xbuf[0:el * 4, :], u_all[OWN], (((1,), (1,)), ((), ())), preferred_element_type=F32)
        ex = lax.broadcasted_iota(jnp.int32, lg.shape, 0)
        lj = [jnp.sum(jnp.where(ex == idx_ref[j], lg, 0.0), axis=0, keepdims=True) for j in range(top)]
        mx = lj[0]
        for j in range(1, top):
            mx = jnp.maximum(mx, lj[j])
        ej = [jnp.exp(v - mx) for v in lj]
        tot = ej[0]
        for j in range(1, top):
            tot = tot + ej[j]
        mrow[OWN] = jnp.zeros((16, t), F32)
        for j in range(top):
            mrow[OWN, j:j + 1, :] = (idx_ref[j] * cap + slot_ref[j]).astype(F32)
            mrow[OWN, 8 + j:9 + j, :] = ej[j] / tot
        m_copies = [rcopy(mrow.at[OWN], mrow.at[role], ms.at[role - 1], mr.at[role - 1], dev)
                    for role, dev in ((SIB, sib), (CROSS, cross), (DIAG, diag))]
        for c in m_copies:
            c.start()
        for i in range(UC // 2, UC):
            u_cross(i).start()
            u_sib(i).start()

        def qkv(k, rope):
            a_dense(k).wait()

            for n in range(2):
                y = _dot(halves(6), ring_a[k % NA, :, n * 512:(n + 1) * 512])
                for h in range(4):
                    yh = y[:, h * HEAD:(h + 1) * HEAD]
                    if rope:
                        yh = yh * macc[4, :, 0:HEAD] + pltpu.roll(yh, HEAD // 2, 1) * macc[5, :, 0:HEAD]
                    col = n * 512 + h * HEAD
                    he[k * t:(k + 1) * t, col:col + HEAD] = yh.astype(BF16)

        for k in range(6):
            qkv(k, k < 4)
            if k < 4:
                a_dense(k + NA).start()
            else:
                a_expert(0, k % NA, 0).start()
                a_expert(0, k % NA, 1).start()
        relay(0)
        for i in range(NB):
            b_ue2(i, i).start()

        ri = lax.broadcasted_iota(jnp.int32, (t, t), 0)
        ci = lax.broadcasted_iota(jnp.int32, (t, t), 1)

        def head_pair(hp, _):
            for s in range(2):
                half = lax.div(hp, nh // 4)
                col = pl.ds(pl.multiple_of((lax.rem(hp, nh // 4) * 2 + s) * HEAD, HEAD), HEAD)
                rq, rk, rv = (pl.ds(pl.multiple_of((2 * kind + half) * t, t), t) for kind in range(3))
                q = he[rq, col]
                kk = he[rk, col]
                vv = he[rv, col]
                sc = lax.dot_general(q, kk, (((1,), (1,)), ((), ())), preferred_element_type=F32) * HEAD ** -0.5
                sc = jnp.where(ri >= ci, sc, -1e30)
                p = jnp.exp(sc - jnp.max(sc, axis=-1, keepdims=True))
                p = (p / jnp.sum(p, axis=-1, keepdims=True)).astype(BF16)
                he[rq, col] = _dot(p, vv).astype(BF16)
            return 0

        lax.fori_loop(0, nh // 2, head_pair, 0)
        relay(1)

        for k in (6, 7):
            a_dense(k).wait()

            for n in range(2):
                col = slice((k % 2) * (d // 2) + n * 512, (k % 2) * (d // 2) + (n + 1) * 512)
                y = _dot(halves(0), ring_a[k % NA, :, n * 512:(n + 1) * 512])
                h0v[:, col] = (h0v[:, col].astype(F32) + y).astype(BF16)
            a_expert(1, k % NA, 0).start()
            a_expert(1, k % NA, 1).start()

        for c in m_copies:
            c.wait()
        for role in range(4):
            macc[role, :, 0:128] = jnp.transpose(jnp.concatenate([mrow[role], jnp.zeros((112, t), F32)], axis=0))
        for i in range(2, UC):
            relay(i)
        for i in range(UC):
            u_sib(i).wait()
        for sl in range(NB):
            b_ue2(sl, sl).wait()

        def swiglu(lhs, sl, dr, between=()):
            between = list(between)
            for n0 in range(0, fe - fe % 256, 256):
                cols = slice(n0, n0 + 256)
                y1 = _dot(lhs(), ring_a[sl, :, cols])
                y3 = _dot(lhs(), ring_a[sl + 1, :, cols])
                he[dr, cols] = (y1 * jax.nn.sigmoid(y1) * y3).astype(BF16)
                if between:
                    between.pop(0)()
            if fe % 256:
                cols = slice(fe - fe % 256, fe)
                y = _dot(lhs(), jnp.concatenate([ring_a[sl, :, cols], ring_a[sl + 1, :, cols]], axis=1))
                y1, y3 = y[:, :fe % 256], y[:, fe % 256:]
                he[dr, cols] = (y1 * jax.nn.sigmoid(y1) * y3).astype(BF16)

        def gather(e, buf, role):
            rr = (lax.broadcasted_iota(jnp.int32, (cap, t), 0) + e * cap).astype(F32) + base
            hit = rr == mrow[role, 0:1, :]
            for j in range(1, top):
                hit = hit | (rr == mrow[role, j:j + 1, :])
            oh = jnp.where(hit, 1.0, 0.0).astype(BF16)
            r0 = buf * rows + role * cap
            for n in range(d // 512):
                xbuf[r0:r0 + cap, n * 512:(n + 1) * 512] = _dot(oh, u_all[role, :, n * 512:(n + 1) * 512]).astype(BF16)

        npart = 4 * t // el
        def gate_part(i):
            role = lax.div(i, el // 4)
            r = pl.ds(pl.multiple_of(lax.rem(i, el // 4) * npart, npart), npart)
            for b in range(rl // 256):
                rr = (lax.broadcasted_iota(jnp.int32, (npart, 256), 1) + b * 256).astype(F32) + base
                w = jnp.zeros((npart, 256), F32)
                for j in range(top):
                    w = jnp.where(rr == macc[role, r, j:j + 1], macc[role, r, 8 + j:9 + j], w)
                for part in range(3):
                    piece = w.astype(BF16)
                    comb[role, r, part * rl + b * 256:part * rl + (b + 1) * 256] = piece
                    w = w - piece.astype(F32)

        for role in (OWN, SIB, CROSS):
            gather(0, 0, role)
        for i in range(UC):
            u_cross(i).wait_send()
            u_fwd(i).wait()
        gather(0, 0, DIAG)

        def y_first(e):
            y = _dot(he[pl.ds(pl.multiple_of(e * rows, 16), rows), :], ring_b[lax.div(e, EB), lax.rem(e, EB)])
            y = y.astype(BF16)
            for role in range(4):
                ybuf[pl.ds(pl.multiple_of(e * cap, 16), cap), role * CC:(role + 1) * CC] = y[role * cap:(role + 1) * cap, :]

        def expert(e, s, last):
            sls = (2 * s, 2 * s + 1)
            for h in range(1 if last else 2):
                for sl in sls:
                    a_expert(e, sl, h).wait()
            y_first(e - 1 if isinstance(e, int) else jnp.maximum(e - 1, 0))
            gate_part(e)

            def refill(h):
                for sl in sls:
                    a_expert(e + 2, sl, h).start()

            def step(k):
                if not last or s == 0:
                    gather(e + 1, 1 - s, k)
                if (k + 1) * 256 == fh:
                    if last:
                        for sl in sls:
                            a_expert(e, sl, 1).wait()
                    else:
                        refill(0)

            swiglu(lambda: xbuf[s * rows:(s + 1) * rows, :], 2 * s, pl.ds(pl.multiple_of(e * rows, 16), rows),
                   [lambda k=k: step(k) for k in range(4)])
            if not last:
                refill(1)

        def pair(p, _):
            for s in range(2):
                expert(p * 2 + s, s, False)
            return 0

        lax.fori_loop(0, el // 2 - 1, pair, 0)
        for sl in range(NB - 1):
            b_ue2(NB + sl, sl).start()
        for s in range(2):
            expert(el - 2 + s, s, True)

        def norm_a(c):
            nr = t // nch
            r = pl.ds(pl.multiple_of(c * nr, nr), nr)
            x = h0v[r, :].astype(F32)
            n = x * lax.rsqrt(jnp.mean(x * x, axis=-1, keepdims=True) + EPS)
            u_all[0, r, :] = (n * ln_ref[1:2, :]).astype(BF16)

        def c_diag(c):
            return rcopy(sdiag, rdiag.at[c], cs_diag.at[c], cr_diag.at[c], sib)

        def c_sib(c):
            return rcopy(ssib, rsib.at[lax.rem(c, 2)], cs_sib.at[c], cr_sib.at[c], sib)

        def c_cross(c):
            return rcopy(rdiag.at[c], rcross.at[c], cs_cross.at[c], cr_cross.at[c], cross)

        def partial(role):
            yc = ybuf[:, role * CC:(role + 1) * CC]
            return _dot(comb[role], jnp.concatenate([yc, yc, yc], axis=0))

        def exchange(c):
            sdiag[...] = partial(DIAG)
            ssib[...] = partial(SIB)
            c_diag(c).start()
            c_sib(c).start()
            pcs[...] = partial(CROSS)
            macc[c] = partial(OWN)

        def finish(c):
            c_diag(c).wait_recv()
            rdiag[c] = rdiag[c] + pcs[...]
            c_cross(c).start()
            c_sib(c).wait_recv()
            macc[c] = macc[c] + rsib[lax.rem(c, 2)]

        def chunk(c, _):
            @pl.when(c <= 2 * nf)
            def _():
                for k in range(2 * nf):
                    @pl.when(c == k + 1)
                    def _():
                        a_shared(k).start()

            for blk in range(2):
                slots = range(blk * (NB // 2), (blk + 1) * (NB // 2))
                for sl in slots:
                    b_ue2(c * NB + sl, sl).wait()
                if blk == 1:
                    norm_a(c)
                for sl in slots:
                    for s in range(EB):
                        e = sl * EB + s
                        y = _dot(he[e * rows:(e + 1) * rows, :], ring_b[sl, s]).astype(BF16)
                        for role in range(4):
                            ybuf[e * cap:(e + 1) * cap, role * CC:(role + 1) * CC] = y[role * cap:(role + 1) * cap, :]

                @pl.when(c + 1 < nch)
                def _():
                    for sl in slots:
                        b_ue2((c + 1) * NB + sl, sl).start()

                @pl.when(c + 1 == nch)
                def _():
                    for sl in slots:
                        for cp in b_ws2(nue2 + sl, sl):
                            cp.start()

                if blk == 0:
                    @pl.when(c >= 2)
                    def _():
                        finish(c - 1)

            c_diag(c - 1).wait_send()
            c_sib(c - 1).wait_send()
            exchange(c)

            @pl.when(c == nch - 1)
            def _():
                finish(c)
            return 0

        y_first(el - 1)
        norm_a(0)
        b_ue2(2 * NB - 1, NB - 1).start()
        exchange(0)
        finish(0)
        lax.fori_loop(1, nch, chunk, 0)

        for half in range(nf):
            a_shared(2 * half).wait()
            a_shared(2 * half + 1).wait()
            swiglu(lambda: u_all[0], 2 * half, slice(half * t, (half + 1) * t))

        for k in range(nws2):
            for cp in b_ws2(nue2 + k, k):
                cp.wait()

        def shared_out(k, _):
            for u in range(cpt):
                f = macc[k * cpt + u]
                for half in range(nf):
                    f = f + _dot(he[half * t:(half + 1) * t, :], ring_b[k, u * nf + half])
                macc[k * cpt + u] = f
            return 0

        lax.fori_loop(0, nws2, shared_out, 0)
        for c in range(nch):
            cols = slice(c * CC, (c + 1) * CC)
            c_cross(c).wait_recv()

            def fin(k, _):
                r = pl.ds(pl.multiple_of(k * 32, 32), 32)
                u_all[1, r, cols] = (h0v[r, cols].astype(F32) + macc[c, r] + rcross[c, r]).astype(BF16)
                return 0

            lax.fori_loop(0, t // 32, fin, 0)
            pltpu.make_async_copy(u_all.at[1, :, pl.ds(c * CC, CC)], out_hbm.at[:, pl.ds(c * CC, CC)],
                                  sem_out.at[c]).start()
        for c in range(nch):
            if c == nch - 1:
                c_diag(c).wait_send()
                c_sib(c).wait_send()
            c_cross(c).wait_send()
            pltpu.make_async_copy(u_all.at[1, :, pl.ds(c * CC, CC)], out_hbm.at[:, pl.ds(c * CC, CC)],
                                  sem_out.at[c]).wait()

    dma = pltpu.SemaphoreType.DMA
    vm = pltpu.VMEM
    any_ = pl.BlockSpec(memory_space=pl.ANY)
    return pl.pallas_call(
        kernel,
        out_shape=jax.ShapeDtypeStruct((t, d), BF16),
        in_specs=[any_] * 19,
        out_specs=any_,
        scratch_shapes=[
            vm((top, 1, t), jnp.int32), vm((top, 1, t), jnp.int32),
            vm((3, d // 128, 128), BF16),
            vm((NA, d, fe), BF16),
            vm((NB, EB, fe, CC), BF16),
            vm((4, t, d), BF16),
            vm((4, t, 3 * rl), BF16),
            vm((2 * rows, d), BF16),
            vm((rl, 4 * CC), BF16),
            vm((el * rows, fe), BF16),
            vm((8, d), F32),
            vm((t, d), BF16),
            vm((4, 16, t), F32),
            vm((nch, t, CC), F32),
            vm((2, t, CC), F32),
            vm((nch, t, CC), F32),
            vm((nch, t, CC), F32),
            vm((t, CC), F32),
            vm((t, CC), F32),
            vm((t, CC), F32),
            dma((NA, 2)), dma((NB, EB)), dma((UC,)), dma((8,)), dma((nch,)),
            dma((3,)), dma((3,)),
            dma((UC,)), dma((UC,)), dma((UC,)), dma((UC,)), dma((UC,)), dma((UC,)),
            dma((nch,)), dma((nch,)), dma((nch,)), dma((nch,)), dma((nch,)), dma((nch,)),
        ],
        compiler_params=pltpu.CompilerParams(collective_id=0, has_side_effects=True,
                                             vmem_limit_bytes=67043328),
        name='moe_layer',
    )


def solution(mesh):
    g_ = mesh.shape['ep']
    rows = P(('dp', 'ep'))
    rep = P()

    def local(h0, idx, slot, ln_attn, wq, wk, wv, wo, ln_ffn, ws1, ws3, ws2, ln_moe, wr, ue1, ue3, ue2):
        b, s, d = h0.shape
        top = idx.shape[-1]
        el, _, fe = ue1.shape
        t = b * s
        cap = CAP_FACTOR * t * top // (el * g_)
        cos, sin = _rope_tables(s)
        gains = [w.reshape(d // 128, 128) for w in (ln_attn, ln_ffn, ln_moe)]
        ids = [jnp.transpose(a, (2, 0, 1)).reshape(top, 1, t) for a in (idx, slot)]
        call = _build(t, d, fe, ws1.shape[1], el, cap, top)
        out = call(h0.reshape(t, d), *ids, *gains, cos, sin, wr.T,
                   wq, wk, wv, wo, ws1, ws3, ws2, ue1, ue3, ue2)
        return out.reshape(b, s, d)

    specs = (rows, rows, rows) + (rep,) * 11 + (P('ep'), P('ep'), P('ep'))
    return jax.shard_map(local, mesh=mesh, in_specs=specs, out_specs=rows, check_vma=False)
```

```python
import jax
import jax.numpy as jnp
import numpy as np
from jax import lax
from jax.experimental import pallas as pl
from jax.experimental.pallas import tpu as pltpu
from jax.sharding import PartitionSpec as P

MESH = pl.DeviceIdType.MESH
F32 = jnp.float32
BF16 = jnp.bfloat16
EPS = 1e-6
HEAD = 128
CAP_FACTOR = 2

OWN, SIB, CROSS, DIAG = range(4)
NA = 4
NB = 4
EB = 4
CC = 256
UC = 4


def _dot(a, b):
    return jnp.dot(a, b, preferred_element_type=F32)


def _rope_tables(s):
    half = HEAD // 2
    freq = np.float32(10000.0) ** (-np.arange(half, dtype=np.float32) / np.float32(half))
    ang = np.arange(s, dtype=np.float32)[:, None] * freq.astype(np.float32)[None, :]
    c, sn = np.cos(ang), np.sin(ang)
    return np.concatenate([c, c], 1).astype(np.float32), np.concatenate([-sn, sn], 1).astype(np.float32)


def _build(t, d, fe, fs, el, cap, top):
    nh = d // HEAD
    rows = 4 * cap
    rl = el * cap
    nch = d // CC
    uc = t // UC
    nta = 8 + 2 * el
    nue2 = nch * el // EB
    dh = d // 2
    fh = fe // 2 // 256 * 256 + 256
    nf = fs // fe
    cpt = EB // nf
    nws2 = nch // cpt
    assert el == NB * EB and nws2 == NB

    def kernel(h0_hbm, idx_hbm, slot_hbm, lna_hbm, lnf_hbm, lnm_hbm, cos_hbm, sin_hbm, wr_hbm, wq, wk, wv, wo, ws1, ws3, ws2,
               ue1, ue3, ue2, out_hbm,
               idx_ref, slot_ref, gain_ref,
               ring_a, ring_b, u_all, comb, xbuf, ybuf, he, ln_ref, h0v, mrow,
               macc, rsib, rcross, rdiag, sdiag, ssib, pcs,
               sem_a, sem_b, sem_in, sem_small, sem_out,
               ms, mr, us_sib, ur_sib, us_cross, ur_cross, us_fwd, ur_diag,
               cs_diag, cr_diag, cs_sib, cr_sib, cs_cross, cr_cross):
        me = lax.axis_index('ep')
        core = lax.rem(me, 2)
        sib = me + 1 - 2 * core
        cross = lax.rem(me + 2, 4)
        diag = lax.rem(sib + 2, 4)
        base = (me * rl).astype(F32)

        def rcopy(src, dst, ssem, rsem, dev):
            return pltpu.make_async_remote_copy(src_ref=src, dst_ref=dst, send_sem=ssem, recv_sem=rsem,
                                                device_id={'ep': dev}, device_id_type=MESH)

        def a_dense(k):
            w = (wq, wk, wv, wo)[k // 2]
            return pltpu.make_async_copy(w.at[:, pl.ds((k % 2) * (d // 2), d // 2)],
                                         ring_a.at[k % NA, :, pl.ds(0, d // 2)], sem_a.at[k % NA, 0])

        def a_expert(e, s, h):
            cols = pl.ds(h * fh, (fh, fe - fh)[h])
            return pltpu.make_async_copy((ue1, ue3)[s % 2].at[e, :, cols], ring_a.at[s, :, cols], sem_a.at[s, h])

        def a_shared(k):
            return pltpu.make_async_copy((ws1, ws3)[k % 2].at[:, pl.ds((k // 2) * fe, fe)],
                                         ring_a.at[k], sem_a.at[k, 0])

        def b_ue2(i, sl):
            e0 = lax.rem(i, el // EB) * EB
            col = pl.multiple_of(lax.div(i, el // EB) * CC, CC)
            return pltpu.make_async_copy(ue2.at[pl.ds(e0, EB), :, pl.ds(col, CC)], ring_b.at[sl], sem_b.at[sl, 0])

        def b_ws2(i, sl):
            k = i - nue2
            return [pltpu.make_async_copy(
                ws2.at[pl.ds(half * fe, fe), pl.ds(pl.multiple_of((k * cpt + u) * CC, CC), CC)],
                ring_b.at[sl, u * nf + half], sem_b.at[sl, u * nf + half])
                for u in range(cpt) for half in range(nf)]

        h0_in = [pltpu.make_async_copy(h0_hbm.at[pl.ds(i * uc, uc)], h0v.at[pl.ds(i * uc, uc)], sem_in.at[i])
                 for i in range(UC)]
        small = [pltpu.make_async_copy(a, b, sem_small.at[i]) for i, (a, b) in enumerate((
            (lna_hbm, gain_ref.at[0]), (lnf_hbm, gain_ref.at[1]), (lnm_hbm, gain_ref.at[2]), (idx_hbm, idx_ref),
            (slot_hbm, slot_ref), (wr_hbm, xbuf.at[pl.ds(0, el * 4)]), (cos_hbm, macc.at[4, :, pl.ds(0, HEAD)]),
            (sin_hbm, macc.at[5, :, pl.ds(0, HEAD)])))]
        for cp in small[:3] + h0_in + small[3:]:
            cp.start()
        bar = pltpu.get_barrier_semaphore()
        for dev in (sib, cross, diag):
            pl.semaphore_signal(bar, inc=1, device_id={'ep': dev}, device_id_type=MESH)
        for k in range(3):
            small[k].wait()
        for k in range(3):
            w = gain_ref[k].astype(F32)
            for i in range(d // 128):
                ln_ref[k:k + 1, i * 128:(i + 1) * 128] = w[i:i + 1, :]

        def u_sib(i):
            r = pl.ds(i * uc, uc)
            return rcopy(u_all.at[OWN, r], u_all.at[SIB, r], us_sib.at[i], ur_sib.at[i], sib)

        def u_cross(i):
            r = pl.ds(i * uc, uc)
            return rcopy(u_all.at[OWN, r], u_all.at[CROSS, r],
                         us_cross.at[i], ur_cross.at[i], cross)

        def u_fwd(i):
            r = pl.ds(i * uc, uc)
            return rcopy(u_all.at[CROSS, r], u_all.at[DIAG, r],
                         us_fwd.at[i], ur_diag.at[i], sib)

        def relay(i):
            u_cross(i).wait_recv()
            u_fwd(i).start()

        def norm_in(k, _):
            r = pl.ds(pl.multiple_of(k * 16, 16), 16)
            x = h0v[r, :].astype(F32)
            n = x * lax.rsqrt(jnp.mean(x * x, axis=-1, keepdims=True) + EPS)
            u_all[OWN, r, :] = (n * ln_ref[2:3, :]).astype(BF16)
            x1 = (n * ln_ref[0:1, :]).astype(BF16)
            for half in range(2):
                he[pl.ds(pl.multiple_of((6 + half) * t + k * 16, 16), 16), 0:dh] = x1[:, half * dh:(half + 1) * dh]
            return 0

        def halves(k):
            return jnp.concatenate([he[k * t:(k + 1) * t, 0:dh], he[(k + 1) * t:(k + 2) * t, 0:dh]], axis=1)

        for i in range(UC):
            h0_in[i].wait()
            if i == 1:
                for k in range(NA):
                    a_dense(k).start()
            lax.fori_loop(i * uc // 16, (i + 1) * uc // 16, norm_in, 0)
            if i == 0:
                pl.semaphore_wait(bar, 3)
            if i < UC // 2:
                u_cross(i).start()
                u_sib(i).start()
        for k in range(3, 8):
            small[k].wait()

        lg = lax.dot_general(xbuf[0:el * 4, :], u_all[OWN], (((1,), (1,)), ((), ())), preferred_element_type=F32)
        ex = lax.broadcasted_iota(jnp.int32, lg.shape, 0)
        lj = [jnp.sum(jnp.where(ex == idx_ref[j], lg, 0.0), axis=0, keepdims=True) for j in range(top)]
        mx = lj[0]
        for j in range(1, top):
            mx = jnp.maximum(mx, lj[j])
        ej = [jnp.exp(v - mx) for v in lj]
        tot = ej[0]
        for j in range(1, top):
            tot = tot + ej[j]
        mrow[OWN] = jnp.zeros((16, t), F32)
        for j in range(top):
            mrow[OWN, j:j + 1, :] = (idx_ref[j] * cap + slot_ref[j]).astype(F32)
            mrow[OWN, 8 + j:9 + j, :] = ej[j] / tot
        m_sib, m_cross, m_fwd = [rcopy(mrow.at[a], mrow.at[b], ms.at[b - 1], mr.at[b - 1], dev)
                                 for a, b, dev in ((OWN, SIB, sib), (OWN, CROSS, cross), (CROSS, DIAG, sib))]
        m_cross.start()
        m_sib.start()
        for i in range(UC // 2, UC):
            u_cross(i).start()
            u_sib(i).start()

        def qkv(k, rope):
            a_dense(k).wait()

            for n in range(2):
                y = _dot(halves(6), ring_a[k % NA, :, n * 512:(n + 1) * 512])
                for h in range(4):
                    yh = y[:, h * HEAD:(h + 1) * HEAD]
                    if rope:
                        yh = yh * macc[4, :, 0:HEAD] + pltpu.roll(yh, HEAD // 2, 1) * macc[5, :, 0:HEAD]
                    col = n * 512 + h * HEAD
                    he[k * t:(k + 1) * t, col:col + HEAD] = yh.astype(BF16)

        for k in range(6):
            qkv(k, k < 4)
            if k < 4:
                a_dense(k + NA).start()
            else:
                a_expert(0, k % NA, 0).start()
                a_expert(0, k % NA, 1).start()
        relay(0)
        for i in range(NB):
            b_ue2(i, i).start()

        ri = lax.broadcasted_iota(jnp.int32, (t, t), 0)
        ci = lax.broadcasted_iota(jnp.int32, (t, t), 1)

        def head_pair(hp, _):
            for s in range(2):
                half = lax.div(hp, nh // 4)
                col = pl.ds(pl.multiple_of((lax.rem(hp, nh // 4) * 2 + s) * HEAD, HEAD), HEAD)
                rq, rk, rv = (pl.ds(pl.multiple_of((2 * kind + half) * t, t), t) for kind in range(3))
                q = he[rq, col]
                kk = he[rk, col]
                vv = he[rv, col]
                sc = lax.dot_general(q, kk, (((1,), (1,)), ((), ())), preferred_element_type=F32) * HEAD ** -0.5
                sc = jnp.where(ri >= ci, sc, -1e30)
                p = jnp.exp(sc - jnp.max(sc, axis=-1, keepdims=True))
                p = (p / jnp.sum(p, axis=-1, keepdims=True)).astype(BF16)
                he[rq, col] = _dot(p, vv).astype(BF16)
            return 0

        lax.fori_loop(0, nh // 2, head_pair, 0)
        m_cross.wait_recv()
        m_fwd.start()
        relay(1)

        def onehot(e, role):
            rr = (lax.broadcasted_iota(jnp.int32, (cap, t), 0) + e * cap).astype(F32) + base
            hit = rr == mrow[role, 0:1, :]
            for j in range(1, top):
                hit = hit | (rr == mrow[role, j:j + 1, :])
            return jnp.where(hit, 1.0, 0.0).astype(BF16)

        def gather(e, buf, role):
            oh = onehot(e, role)
            r0 = buf * rows + role * cap
            for n in range(d // 512):
                xbuf[r0:r0 + cap, n * 512:(n + 1) * 512] = _dot(oh, u_all[role, :, n * 512:(n + 1) * 512]).astype(BF16)

        def gather_first(role):
            oh = jnp.concatenate([onehot(0, role)] + [onehot(2 * p + 1, role) for p in range(el // 2)], axis=0)
            for n in range(d // 512):
                x = _dot(oh, u_all[role, :, n * 512:(n + 1) * 512]).astype(BF16)
                xbuf[role * cap:(role + 1) * cap, n * 512:(n + 1) * 512] = x[0:cap, :]
                half, col = divmod(n * 512, dh)
                for p in range(el // 2):
                    r0 = (2 * p + half) * rows + role * cap
                    he[r0:r0 + cap, col:col + 512] = x[(p + 1) * cap:(p + 2) * cap, :]

        for k in (6, 7):
            a_dense(k).wait()

            for n in range(2):
                col = slice((k % 2) * (d // 2) + n * 512, (k % 2) * (d // 2) + (n + 1) * 512)
                y = _dot(halves(0), ring_a[k % NA, :, n * 512:(n + 1) * 512])
                h0v[:, col] = (h0v[:, col].astype(F32) + y).astype(BF16)
            a_expert(1, k % NA, 0).start()
            a_expert(1, k % NA, 1).start()

        m_sib.wait()
        m_cross.wait_send()
        m_fwd.wait()
        for role in range(4):
            macc[role, :, 0:128] = jnp.transpose(jnp.concatenate([mrow[role], jnp.zeros((112, t), F32)], axis=0))
        for i in range(2, UC - 1):
            relay(i)
        for i in range(UC):
            u_sib(i).wait()
        gather_first(OWN)
        gather_first(SIB)
        relay(UC - 1)
        for sl in range(NB):
            b_ue2(sl, sl).wait()

        def swiglu(lhs, sl, dr, between=()):
            between = list(between)
            for n0 in range(0, fe - fe % 256, 256):
                cols = slice(n0, n0 + 256)
                y1 = _dot(lhs(), ring_a[sl, :, cols])
                y3 = _dot(lhs(), ring_a[sl + 1, :, cols])
                he[dr, cols] = (y1 * jax.nn.sigmoid(y1) * y3).astype(BF16)
                if between:
                    between.pop(0)()
            if fe % 256:
                cols = slice(fe - fe % 256, fe)
                y = sum(_dot(lhs()[:, k:k + dh], jnp.concatenate(
                    [ring_a[sl, k:k + dh, cols], ring_a[sl + 1, k:k + dh, cols]], axis=1)) for k in (0, dh))
                y1, y3 = y[:, :fe % 256], y[:, fe % 256:]
                he[dr, cols] = (y1 * jax.nn.sigmoid(y1) * y3).astype(BF16)

        npart = 4 * t // el
        def gate_part(i):
            role = lax.div(i, el // 4)
            r = pl.ds(pl.multiple_of(lax.rem(i, el // 4) * npart, npart), npart)
            for b in range(rl // 256):
                rr = (lax.broadcasted_iota(jnp.int32, (npart, 256), 1) + b * 256).astype(F32) + base
                w = jnp.zeros((npart, 256), F32)
                for j in range(top):
                    w = jnp.where(rr == macc[role, r, j:j + 1], macc[role, r, 8 + j:9 + j], w)
                for part in range(3):
                    piece = w.astype(BF16)
                    comb[role, r, part * rl + b * 256:part * rl + (b + 1) * 256] = piece
                    w = w - piece.astype(F32)

        gather_first(CROSS)
        for i in range(UC):
            u_cross(i).wait_send()
            u_fwd(i).wait()
        gather_first(DIAG)

        def y_first(e):
            er = pl.ds(pl.multiple_of(e * rows, 16), rows)
            y = sum(_dot(he[er, a:b], ring_b[lax.div(e, EB), lax.rem(e, EB), a:b, :])
                    for a, b in ((0, fh), (fh, fe))).astype(BF16)
            for role in range(4):
                ybuf[pl.ds(pl.multiple_of(e * cap, 16), cap), role * CC:(role + 1) * CC] = y[role * cap:(role + 1) * cap, :]

        def expert(e, s, last):
            sls = (2 * s, 2 * s + 1)
            for h in range(1 if last else 2):
                for sl in sls:
                    a_expert(e, sl, h).wait()
            if s == 0:
                for half in range(2):
                    xbuf[rows:2 * rows, half * dh:(half + 1) * dh] = (
                        he[pl.ds(pl.multiple_of((e + half) * rows, 16), rows), 0:dh])
            y_first(e - 1 if isinstance(e, int) else jnp.maximum(e - 1, 0))
            gate_part(e)

            def refill(h):
                for sl in sls:
                    a_expert(e + 2, sl, h).start()

            def step(k):
                if s == 1 and not last:
                    gather(e + 1, 0, k)
                if (k + 1) * 256 == fh:
                    if last:
                        for sl in sls:
                            a_expert(e, sl, 1).wait()
                    else:
                        refill(0)

            swiglu(lambda: xbuf[s * rows:(s + 1) * rows, :], 2 * s, pl.ds(pl.multiple_of(e * rows, 16), rows),
                   [lambda k=k: step(k) for k in range(4)])
            if not last:
                refill(1)

        def pair(p, _):
            for s in range(2):
                expert(p * 2 + s, s, False)
            return 0

        lax.fori_loop(0, el // 2 - 1, pair, 0)
        for sl in range(NB - 1):
            b_ue2(NB + sl, sl).start()
        for s in range(2):
            expert(el - 2 + s, s, True)

        def norm_a(c):
            nr = t // nch
            r = pl.ds(pl.multiple_of(c * nr, nr), nr)
            x = h0v[r, :].astype(F32)
            n = x * lax.rsqrt(jnp.mean(x * x, axis=-1, keepdims=True) + EPS)
            u_all[0, r, :] = (n * ln_ref[1:2, :]).astype(BF16)

        def c_diag(c):
            return rcopy(sdiag, rdiag.at[c], cs_diag.at[c], cr_diag.at[c], sib)

        def c_sib(c):
            return rcopy(ssib, rsib.at[lax.rem(c, 2)], cs_sib.at[c], cr_sib.at[c], sib)

        def c_cross(c):
            return rcopy(rdiag.at[c], rcross.at[c], cs_cross.at[c], cr_cross.at[c], cross)

        def partial(role):
            yc = ybuf[:, role * CC:(role + 1) * CC]
            return _dot(comb[role], jnp.concatenate([yc, yc, yc], axis=0))

        def exchange(c):
            sdiag[...] = partial(DIAG)
            ssib[...] = partial(SIB)
            c_diag(c).start()
            c_sib(c).start()
            pcs[...] = partial(CROSS)
            macc[c] = partial(OWN)

        def finish(c):
            c_diag(c).wait_recv()
            rdiag[c] = rdiag[c] + pcs[...]
            c_cross(c).start()
            c_sib(c).wait_recv()
            macc[c] = macc[c] + rsib[lax.rem(c, 2)]

        def chunk(c, _):
            @pl.when(c <= 2 * nf)
            def _():
                for k in range(2 * nf):
                    @pl.when(c == k + 1)
                    def _():
                        a_shared(k).start()

            for blk in range(2):
                slots = range(blk * (NB // 2), (blk + 1) * (NB // 2))
                for sl in slots:
                    b_ue2(c * NB + sl, sl).wait()
                if blk == 1:
                    norm_a(c)
                for sl in slots:
                    for s in range(EB):
                        e = sl * EB + s
                        y = _dot(he[e * rows:(e + 1) * rows, :], ring_b[sl, s]).astype(BF16)
                        for role in range(4):
                            ybuf[e * cap:(e + 1) * cap, role * CC:(role + 1) * CC] = y[role * cap:(role + 1) * cap, :]

                @pl.when(c + 1 < nch)
                def _():
                    for sl in slots:
                        b_ue2((c + 1) * NB + sl, sl).start()

                @pl.when(c + 1 == nch)
                def _():
                    for sl in slots:
                        for cp in b_ws2(nue2 + sl, sl):
                            cp.start()

                if blk == 0:
                    @pl.when(c >= 3)
                    def _():
                        finish(c - 1)

            c_diag(c - 1).wait_send()
            c_sib(c - 1).wait_send()
            exchange(c)

            @pl.when((c == 1) | (c == nch - 1))
            def _():
                finish(c)
            return 0

        y_first(el - 1)
        b_ue2(2 * NB - 1, NB - 1).start()
        exchange(0)
        finish(0)
        norm_a(0)
        lax.fori_loop(1, nch, chunk, 0)

        for half in range(nf):
            a_shared(2 * half).wait()
            a_shared(2 * half + 1).wait()
            swiglu(lambda: u_all[0], 2 * half, slice(half * t, (half + 1) * t))

        for k in range(nws2):
            for cp in b_ws2(nue2 + k, k):
                cp.wait()

        def shared_out(k, _):
            for u in range(cpt):
                f = macc[k * cpt + u]
                for half in range(nf):
                    f = f + _dot(he[half * t:(half + 1) * t, :], ring_b[k, u * nf + half])
                macc[k * cpt + u] = f
            return 0

        lax.fori_loop(0, nws2, shared_out, 0)
        for c in range(nch):
            cols = slice(c * CC, (c + 1) * CC)
            c_cross(c).wait_recv()

            def fin(k, _):
                r = pl.ds(pl.multiple_of(k * 32, 32), 32)
                u_all[1, r, cols] = (h0v[r, cols].astype(F32) + macc[c, r] + rcross[c, r]).astype(BF16)
                return 0

            lax.fori_loop(0, t // 32, fin, 0)
            pltpu.make_async_copy(u_all.at[1, :, pl.ds(c * CC, CC)], out_hbm.at[:, pl.ds(c * CC, CC)],
                                  sem_out.at[c]).start()
        for c in range(nch):
            if c == nch - 1:
                c_diag(c).wait_send()
                c_sib(c).wait_send()
            c_cross(c).wait_send()
            pltpu.make_async_copy(u_all.at[1, :, pl.ds(c * CC, CC)], out_hbm.at[:, pl.ds(c * CC, CC)],
                                  sem_out.at[c]).wait()

    dma = pltpu.SemaphoreType.DMA
    vm = pltpu.VMEM
    any_ = pl.BlockSpec(memory_space=pl.ANY)
    return pl.pallas_call(
        kernel,
        out_shape=jax.ShapeDtypeStruct((t, d), BF16),
        in_specs=[any_] * 19,
        out_specs=any_,
        scratch_shapes=[
            vm((top, 1, t), jnp.int32), vm((top, 1, t), jnp.int32),
            vm((3, d // 128, 128), BF16),
            vm((NA, d, fe), BF16),
            vm((NB, EB, fe, CC), BF16),
            vm((4, t, d), BF16),
            vm((4, t, 3 * rl), BF16),
            vm((2 * rows, d), BF16),
            vm((rl, 4 * CC), BF16),
            vm((el * rows, fe), BF16),
            vm((8, d), F32),
            vm((t, d), BF16),
            vm((4, 16, t), F32),
            vm((nch, t, CC), F32),
            vm((2, t, CC), F32),
            vm((nch, t, CC), F32),
            vm((nch, t, CC), F32),
            vm((t, CC), F32),
            vm((t, CC), F32),
            vm((t, CC), F32),
            dma((NA, 2)), dma((NB, EB)), dma((UC,)), dma((8,)), dma((nch,)),
            dma((3,)), dma((3,)),
            dma((UC,)), dma((UC,)), dma((UC,)), dma((UC,)), dma((UC,)), dma((UC,)),
            dma((nch,)), dma((nch,)), dma((nch,)), dma((nch,)), dma((nch,)), dma((nch,)),
        ],
        compiler_params=pltpu.CompilerParams(collective_id=0, has_side_effects=True,
                                             vmem_limit_bytes=67043328),
        name='moe_layer',
    )


def solution(mesh):
    g_ = mesh.shape['ep']
    rows = P(('dp', 'ep'))
    rep = P()

    def local(h0, idx, slot, ln_attn, wq, wk, wv, wo, ln_ffn, ws1, ws3, ws2, ln_moe, wr, ue1, ue3, ue2):
        b, s, d = h0.shape
        top = idx.shape[-1]
        el, _, fe = ue1.shape
        t = b * s
        cap = CAP_FACTOR * t * top // (el * g_)
        cos, sin = _rope_tables(s)
        gains = [w.reshape(d // 128, 128) for w in (ln_attn, ln_ffn, ln_moe)]
        ids = [jnp.transpose(a, (2, 0, 1)).reshape(top, 1, t) for a in (idx, slot)]
        call = _build(t, d, fe, ws1.shape[1], el, cap, top)
        out = call(h0.reshape(t, d), *ids, *gains, cos, sin, wr.T,
                   wq, wk, wv, wo, ws1, ws3, ws2, ue1, ue3, ue2)
        return out.reshape(b, s, d)

    specs = (rows, rows, rows) + (rep,) * 11 + (P('ep'), P('ep'), P('ep'))
    return jax.shard_map(local, mesh=mesh, in_specs=specs, out_specs=rows, check_vma=False)
```

```python
import jax
import jax.numpy as jnp
import numpy as np
from jax import lax
from jax.experimental import pallas as pl
from jax.experimental.pallas import tpu as pltpu
from jax.sharding import PartitionSpec as P

MESH = pl.DeviceIdType.MESH
F32 = jnp.float32
BF16 = jnp.bfloat16
EPS = 1e-6
HEAD = 128
CAP_FACTOR = 2

OWN, SIB, CROSS, DIAG = range(4)
NA = 4
NB = 4
EB = 4
CC = 256
UC = 4


def _dot(a, b):
    return jnp.dot(a, b, preferred_element_type=F32)


def _rope_tables(s):
    half = HEAD // 2
    freq = np.float32(10000.0) ** (-np.arange(half, dtype=np.float32) / np.float32(half))
    ang = np.arange(s, dtype=np.float32)[:, None] * freq.astype(np.float32)[None, :]
    c, sn = np.cos(ang), np.sin(ang)
    return np.concatenate([c, c], 1).astype(np.float32), np.concatenate([-sn, sn], 1).astype(np.float32)


def _build(t, d, fe, fs, el, cap, top):
    nh = d // HEAD
    rows = 4 * cap
    rl = el * cap
    nch = d // CC
    uc = t // UC
    nta = 8 + 2 * el
    nue2 = nch * el // EB
    dh = d // 2
    fh = fe // 2 // 256 * 256 + 256
    nf = fs // fe
    cpt = EB // nf
    nws2 = nch // cpt
    assert el == NB * EB and nws2 == NB

    def kernel(h0_hbm, idx_hbm, slot_hbm, lna_hbm, lnf_hbm, lnm_hbm, cos_hbm, sin_hbm, wr_hbm, wq, wk, wv, wo, ws1, ws3, ws2,
               ue1, ue3, ue2, out_hbm,
               idx_ref, slot_ref, gain_ref,
               ring_a, ring_b, u_all, comb, xbuf, ybuf, he, ln_ref, h0v, mrow,
               macc, rsib, rcross, rdiag, sdiag, ssib, pcs,
               sem_a, sem_b, sem_in, sem_small, sem_out,
               ms, mr, us_sib, ur_sib, us_cross, ur_cross, us_fwd, ur_diag,
               cs_diag, cr_diag, cs_sib, cr_sib, cs_cross, cr_cross):
        me = lax.axis_index('ep')
        core = lax.rem(me, 2)
        sib = me + 1 - 2 * core
        cross = lax.rem(me + 2, 4)
        diag = lax.rem(sib + 2, 4)
        base = (me * rl).astype(F32)

        def rcopy(src, dst, ssem, rsem, dev):
            return pltpu.make_async_remote_copy(src_ref=src, dst_ref=dst, send_sem=ssem, recv_sem=rsem,
                                                device_id={'ep': dev}, device_id_type=MESH)

        def a_dense(k):
            w = (wq, wk, wv, wo)[k // 2]
            return pltpu.make_async_copy(w.at[:, pl.ds((k % 2) * (d // 2), d // 2)],
                                         ring_a.at[k % NA, :, pl.ds(0, d // 2)], sem_a.at[k % NA, 0])

        def a_expert(e, s, h):
            cols = pl.ds(h * fh, (fh, fe - fh)[h])
            return pltpu.make_async_copy((ue1, ue3)[s % 2].at[e, :, cols], ring_a.at[s, :, cols], sem_a.at[s, h])

        def a_shared(k):
            return pltpu.make_async_copy((ws1, ws3)[k % 2].at[:, pl.ds((k // 2) * fe, fe)],
                                         ring_a.at[k], sem_a.at[k, 0])

        def b_ue2(i, sl):
            e0 = lax.rem(i, el // EB) * EB
            col = pl.multiple_of(lax.div(i, el // EB) * CC, CC)
            return pltpu.make_async_copy(ue2.at[pl.ds(e0, EB), :, pl.ds(col, CC)], ring_b.at[sl], sem_b.at[sl, 0])

        def b_ws2(i, sl):
            k = i - nue2
            return [pltpu.make_async_copy(
                ws2.at[pl.ds(half * fe, fe), pl.ds(pl.multiple_of((k * cpt + u) * CC, CC), CC)],
                ring_b.at[sl, u * nf + half], sem_b.at[sl, u * nf + half])
                for u in range(cpt) for half in range(nf)]

        h0_in = [pltpu.make_async_copy(h0_hbm.at[pl.ds(i * uc, uc)], h0v.at[pl.ds(i * uc, uc)], sem_in.at[i])
                 for i in range(UC)]
        small = [pltpu.make_async_copy(a, b, sem_small.at[i]) for i, (a, b) in enumerate((
            (lna_hbm, gain_ref.at[0]), (lnf_hbm, gain_ref.at[1]), (lnm_hbm, gain_ref.at[2]), (idx_hbm, idx_ref),
            (slot_hbm, slot_ref), (wr_hbm, xbuf.at[pl.ds(0, el * 4)]), (cos_hbm, macc.at[4, :, pl.ds(0, HEAD)]),
            (sin_hbm, macc.at[5, :, pl.ds(0, HEAD)])))]
        for cp in small[:3] + h0_in + small[3:]:
            cp.start()
        bar = pltpu.get_barrier_semaphore()
        for dev in (sib, cross, diag):
            pl.semaphore_signal(bar, inc=1, device_id={'ep': dev}, device_id_type=MESH)
        for k in range(3):
            small[k].wait()
        for k in range(3):
            w = gain_ref[k].astype(F32)
            for i in range(d // 128):
                ln_ref[k:k + 1, i * 128:(i + 1) * 128] = w[i:i + 1, :]

        def u_sib(i):
            r = pl.ds(i * uc, uc)
            return rcopy(u_all.at[OWN, r], u_all.at[SIB, r], us_sib.at[i], ur_sib.at[i], sib)

        def u_cross(i):
            r = pl.ds(i * uc, uc)
            return rcopy(u_all.at[OWN, r], u_all.at[CROSS, r],
                         us_cross.at[i], ur_cross.at[i], cross)

        def u_fwd(i):
            r = pl.ds(i * uc, uc)
            return rcopy(u_all.at[CROSS, r], u_all.at[DIAG, r],
                         us_fwd.at[i], ur_diag.at[i], sib)

        def relay(i):
            u_cross(i).wait_recv()
            u_fwd(i).start()

        def norm_in(k, _):
            r = pl.ds(pl.multiple_of(k * 16, 16), 16)
            x = h0v[r, :].astype(F32)
            n = x * lax.rsqrt(jnp.mean(x * x, axis=-1, keepdims=True) + EPS)
            u_all[OWN, r, :] = (n * ln_ref[2:3, :]).astype(BF16)
            x1 = (n * ln_ref[0:1, :]).astype(BF16)
            for half in range(2):
                he[pl.ds(pl.multiple_of((6 + half) * t + k * 16, 16), 16), 0:dh] = x1[:, half * dh:(half + 1) * dh]
            return 0

        def halves(k):
            return jnp.concatenate([he[k * t:(k + 1) * t, 0:dh], he[(k + 1) * t:(k + 2) * t, 0:dh]], axis=1)

        for i in range(UC):
            h0_in[i].wait()
            if i == 1:
                for k in range(NA):
                    a_dense(k).start()
            lax.fori_loop(i * uc // 16, (i + 1) * uc // 16, norm_in, 0)
            if i == 0:
                pl.semaphore_wait(bar, 3)
            if i < UC // 2:
                u_cross(i).start()
                u_sib(i).start()
        for k in range(3, 8):
            small[k].wait()

        lg = lax.dot_general(xbuf[0:el * 4, :], u_all[OWN], (((1,), (1,)), ((), ())), preferred_element_type=F32)
        ex = lax.broadcasted_iota(jnp.int32, lg.shape, 0)
        lj = [jnp.sum(jnp.where(ex == idx_ref[j], lg, 0.0), axis=0, keepdims=True) for j in range(top)]
        mx = lj[0]
        for j in range(1, top):
            mx = jnp.maximum(mx, lj[j])
        ej = [jnp.exp(v - mx) for v in lj]
        tot = ej[0]
        for j in range(1, top):
            tot = tot + ej[j]
        mrow[OWN] = jnp.zeros((16, t), F32)
        for j in range(top):
            mrow[OWN, j:j + 1, :] = (idx_ref[j] * cap + slot_ref[j]).astype(F32)
            mrow[OWN, 8 + j:9 + j, :] = ej[j] / tot
        m_sib, m_cross, m_fwd = [rcopy(mrow.at[a], mrow.at[b], ms.at[b - 1], mr.at[b - 1], dev)
                                 for a, b, dev in ((OWN, SIB, sib), (OWN, CROSS, cross), (CROSS, DIAG, sib))]
        m_cross.start()
        m_sib.start()
        for i in range(UC // 2, UC):
            u_cross(i).start()
            u_sib(i).start()

        def qkv(k, rope):
            a_dense(k).wait()

            for n in range(2):
                y = _dot(halves(6), ring_a[k % NA, :, n * 512:(n + 1) * 512])
                for h in range(4):
                    yh = y[:, h * HEAD:(h + 1) * HEAD]
                    if rope:
                        yh = yh * macc[4, :, 0:HEAD] + pltpu.roll(yh, HEAD // 2, 1) * macc[5, :, 0:HEAD]
                    col = n * 512 + h * HEAD
                    he[k * t:(k + 1) * t, col:col + HEAD] = yh.astype(BF16)

        for k in range(6):
            qkv(k, k < 4)
            if k < 4:
                a_dense(k + NA).start()
            else:
                a_expert(0, k % NA, 0).start()
                a_expert(0, k % NA, 1).start()
        relay(0)
        for i in range(NB):
            b_ue2(i, i).start()

        ri = lax.broadcasted_iota(jnp.int32, (t, t), 0)
        ci = lax.broadcasted_iota(jnp.int32, (t, t), 1)

        def head_pair(hp, _):
            for s in range(2):
                half = lax.div(hp, nh // 4)
                col = pl.ds(pl.multiple_of((lax.rem(hp, nh // 4) * 2 + s) * HEAD, HEAD), HEAD)
                rq, rk, rv = (pl.ds(pl.multiple_of((2 * kind + half) * t, t), t) for kind in range(3))
                q = he[rq, col]
                kk = he[rk, col]
                vv = he[rv, col]
                sc = lax.dot_general(q, kk, (((1,), (1,)), ((), ())), preferred_element_type=F32) * HEAD ** -0.5
                sc = jnp.where(ri >= ci, sc, -1e30)
                p = jnp.exp(sc - jnp.max(sc, axis=-1, keepdims=True))
                p = (p / jnp.sum(p, axis=-1, keepdims=True)).astype(BF16)
                he[rq, col] = _dot(p, vv).astype(BF16)
            return 0

        lax.fori_loop(0, nh // 2, head_pair, 0)
        m_cross.wait_recv()
        m_fwd.start()
        relay(1)

        def onehot(e, role):
            rr = (lax.broadcasted_iota(jnp.int32, (cap, t), 0) + e * cap).astype(F32) + base
            hit = rr == mrow[role, 0:1, :]
            for j in range(1, top):
                hit = hit | (rr == mrow[role, j:j + 1, :])
            return jnp.where(hit, 1.0, 0.0).astype(BF16)

        def gather(e, buf, role):
            oh = onehot(e, role)
            r0 = buf * rows + role * cap
            for n in range(d // 512):
                xbuf[r0:r0 + cap, n * 512:(n + 1) * 512] = _dot(oh, u_all[role, :, n * 512:(n + 1) * 512]).astype(BF16)

        def gather_first(role):
            oh = jnp.concatenate([onehot(0, role)] + [onehot(2 * p + 1, role) for p in range(el // 2)], axis=0)
            for n in range(d // 512):
                x = _dot(oh, u_all[role, :, n * 512:(n + 1) * 512]).astype(BF16)
                xbuf[role * cap:(role + 1) * cap, n * 512:(n + 1) * 512] = x[0:cap, :]
                half, col = divmod(n * 512, dh)
                for p in range(el // 2):
                    r0 = (2 * p + half) * rows + role * cap
                    he[r0:r0 + cap, col:col + 512] = x[(p + 1) * cap:(p + 2) * cap, :]

        for k in (6, 7):
            a_dense(k).wait()

            for n in range(2):
                col = slice((k % 2) * (d // 2) + n * 512, (k % 2) * (d // 2) + (n + 1) * 512)
                y = _dot(halves(0), ring_a[k % NA, :, n * 512:(n + 1) * 512])
                h0v[:, col] = (h0v[:, col].astype(F32) + y).astype(BF16)
            a_expert(1, k % NA, 0).start()
            a_expert(1, k % NA, 1).start()

        m_sib.wait()
        m_cross.wait_send()
        m_fwd.wait()
        for role in range(4):
            macc[role, :, 0:128] = jnp.transpose(jnp.concatenate([mrow[role], jnp.zeros((112, t), F32)], axis=0))
        for i in range(2, UC - 1):
            relay(i)
        for i in range(UC):
            u_sib(i).wait()
        gather_first(OWN)
        gather_first(SIB)
        relay(UC - 1)
        for sl in range(NB):
            b_ue2(sl, sl).wait()

        def swiglu(lhs, sl, dr, between=()):
            between = list(between)
            for n0 in range(0, fe - fe % 256, 256):
                cols = slice(n0, n0 + 256)
                y1 = _dot(lhs(), ring_a[sl, :, cols])
                y3 = _dot(lhs(), ring_a[sl + 1, :, cols])
                he[dr, cols] = (y1 * jax.nn.sigmoid(y1) * y3).astype(BF16)
                if between:
                    between.pop(0)()
            if fe % 256:
                cols = slice(fe - fe % 256, fe)
                y = sum(_dot(lhs()[:, k:k + dh], jnp.concatenate(
                    [ring_a[sl, k:k + dh, cols], ring_a[sl + 1, k:k + dh, cols]], axis=1)) for k in (0, dh))
                y1, y3 = y[:, :fe % 256], y[:, fe % 256:]
                he[dr, cols] = (y1 * jax.nn.sigmoid(y1) * y3).astype(BF16)

        npart = 4 * t // el
        def gate_part(i):
            role = lax.div(i, el // 4)
            r = pl.ds(pl.multiple_of(lax.rem(i, el // 4) * npart, npart), npart)
            for b in range(rl // 256):
                rr = (lax.broadcasted_iota(jnp.int32, (npart, 256), 1) + b * 256).astype(F32) + base
                w = jnp.zeros((npart, 256), F32)
                for j in range(top):
                    w = jnp.where(rr == macc[role, r, j:j + 1], macc[role, r, 8 + j:9 + j], w)
                for part in range(3):
                    piece = w.astype(BF16)
                    comb[role, r, part * rl + b * 256:part * rl + (b + 1) * 256] = piece
                    w = w - piece.astype(F32)

        gather_first(CROSS)
        for i in range(UC):
            u_cross(i).wait_send()
            u_fwd(i).wait()
        gather_first(DIAG)

        def y_first(e):
            er = pl.ds(pl.multiple_of(e * rows, 16), rows)
            y = sum(_dot(he[er, a:b], ring_b[lax.div(e, EB), lax.rem(e, EB), a:b, :])
                    for a, b in ((0, fh), (fh, fe))).astype(BF16)
            for role in range(4):
                ybuf[pl.ds(pl.multiple_of(e * cap, 16), cap), role * CC:(role + 1) * CC] = y[role * cap:(role + 1) * cap, :]

        def expert(e, s, last):
            sls = (2 * s, 2 * s + 1)
            for h in range(2):
                for sl in sls:
                    a_expert(e, sl, h).wait()
            if s == 0:
                for half in range(2):
                    xbuf[rows:2 * rows, half * dh:(half + 1) * dh] = (
                        he[pl.ds(pl.multiple_of((e + half) * rows, 16), rows), 0:dh])
            y_first(e - 1 if isinstance(e, int) else jnp.maximum(e - 1, 0))
            gate_part(e)

            def refill(h):
                for sl in sls:
                    a_expert(e + 2, sl, h).start()

            def step(k):
                if s == 1 and not last:
                    gather(e + 1, 0, k)
                if (k + 1) * 256 == fh and not last:
                    refill(0)

            swiglu(lambda: xbuf[s * rows:(s + 1) * rows, :], 2 * s, pl.ds(pl.multiple_of(e * rows, 16), rows),
                   [lambda k=k: step(k) for k in range(4)])
            if not last:
                refill(1)

        def pair(p, _):
            for s in range(2):
                expert(p * 2 + s, s, False)
            return 0

        lax.fori_loop(0, el // 2 - 1, pair, 0)
        for sl in range(NB - 1):
            b_ue2(NB + sl, sl).start()
        for s in range(2):
            expert(el - 2 + s, s, True)

        def norm_a(c):
            nr = t // nch
            r = pl.ds(pl.multiple_of(c * nr, nr), nr)
            x = h0v[r, :].astype(F32)
            n = x * lax.rsqrt(jnp.mean(x * x, axis=-1, keepdims=True) + EPS)
            u_all[0, r, :] = (n * ln_ref[1:2, :]).astype(BF16)

        def c_diag(c):
            return rcopy(sdiag, rdiag.at[c], cs_diag.at[c], cr_diag.at[c], sib)

        def c_sib(c):
            return rcopy(ssib, rsib.at[lax.rem(c, 2)], cs_sib.at[c], cr_sib.at[c], sib)

        def c_cross(c):
            return rcopy(rdiag.at[c], rcross.at[c], cs_cross.at[c], cr_cross.at[c], cross)

        def partial(role):
            yc = ybuf[:, role * CC:(role + 1) * CC]
            return _dot(comb[role], jnp.concatenate([yc, yc, yc], axis=0))

        def exchange(c):
            sdiag[...] = partial(DIAG)
            ssib[...] = partial(SIB)
            c_diag(c).start()
            c_sib(c).start()
            pcs[...] = partial(CROSS)
            macc[c] = partial(OWN)

        def send_cross(c):
            c_diag(c).wait_recv()
            rdiag[c] = rdiag[c] + pcs[...]
            c_cross(c).start()

        def add_sib(c):
            c_sib(c).wait_recv()
            macc[c] = macc[c] + rsib[lax.rem(c, 2)]

        def chunk(c, _):
            @pl.when(c <= 2 * nf)
            def _():
                for k in range(2 * nf):
                    @pl.when(c == k + 1)
                    def _():
                        a_shared(k).start()

            for blk in range(2):
                slots = range(blk * (NB // 2), (blk + 1) * (NB // 2))
                for sl in slots:
                    b_ue2(c * NB + sl, sl).wait()
                if blk == 1:
                    norm_a(c)
                for sl in slots:
                    for s in range(EB):
                        e = sl * EB + s
                        y = _dot(he[e * rows:(e + 1) * rows, :], ring_b[sl, s]).astype(BF16)
                        for role in range(4):
                            ybuf[e * cap:(e + 1) * cap, role * CC:(role + 1) * CC] = y[role * cap:(role + 1) * cap, :]

                @pl.when(c + 1 < nch)
                def _():
                    for sl in slots:
                        b_ue2((c + 1) * NB + sl, sl).start()

                @pl.when(c + 1 == nch)
                def _():
                    for sl in slots:
                        for cp in b_ws2(nue2 + sl, sl):
                            cp.start()

                if blk == 0:
                    @pl.when(c >= 4)
                    def _():
                        send_cross(c - 1)

                    add_sib(c - 1)

            c_diag(c - 1).wait_send()
            c_sib(c - 1).wait_send()
            exchange(c)

            @pl.when((c <= 2) | (c == nch - 1))
            def _():
                send_cross(c)
            return 0

        y_first(el - 1)
        b_ue2(2 * NB - 1, NB - 1).start()
        exchange(0)
        send_cross(0)
        norm_a(0)
        lax.fori_loop(1, nch, chunk, 0)
        add_sib(nch - 1)

        for half in range(nf):
            a_shared(2 * half).wait()
            a_shared(2 * half + 1).wait()
            swiglu(lambda: u_all[0], 2 * half, slice(half * t, (half + 1) * t))

        for k in range(nws2):
            for cp in b_ws2(nue2 + k, k):
                cp.wait()

        def shared_out(k, _):
            for u in range(cpt):
                f = macc[k * cpt + u]
                for half in range(nf):
                    f = f + _dot(he[half * t:(half + 1) * t, :], ring_b[k, u * nf + half])
                macc[k * cpt + u] = f
            return 0

        lax.fori_loop(0, nws2, shared_out, 0)
        for c in range(nch):
            cols = slice(c * CC, (c + 1) * CC)
            c_cross(c).wait_recv()

            def fin(k, _):
                r = pl.ds(pl.multiple_of(k * 32, 32), 32)
                u_all[1, r, cols] = (h0v[r, cols].astype(F32) + macc[c, r] + rcross[c, r]).astype(BF16)
                return 0

            lax.fori_loop(0, t // 32, fin, 0)
            pltpu.make_async_copy(u_all.at[1, :, pl.ds(c * CC, CC)], out_hbm.at[:, pl.ds(c * CC, CC)],
                                  sem_out.at[c]).start()
        for c in range(nch):
            if c == nch - 1:
                c_diag(c).wait_send()
                c_sib(c).wait_send()
            c_cross(c).wait_send()
            pltpu.make_async_copy(u_all.at[1, :, pl.ds(c * CC, CC)], out_hbm.at[:, pl.ds(c * CC, CC)],
                                  sem_out.at[c]).wait()

    dma = pltpu.SemaphoreType.DMA
    vm = pltpu.VMEM
    any_ = pl.BlockSpec(memory_space=pl.ANY)
    return pl.pallas_call(
        kernel,
        out_shape=jax.ShapeDtypeStruct((t, d), BF16),
        in_specs=[any_] * 19,
        out_specs=any_,
        scratch_shapes=[
            vm((top, 1, t), jnp.int32), vm((top, 1, t), jnp.int32),
            vm((3, d // 128, 128), BF16),
            vm((NA, d, fe), BF16),
            vm((NB, EB, fe, CC), BF16),
            vm((4, t, d), BF16),
            vm((4, t, 3 * rl), BF16),
            vm((2 * rows, d), BF16),
            vm((rl, 4 * CC), BF16),
            vm((el * rows, fe), BF16),
            vm((8, d), F32),
            vm((t, d), BF16),
            vm((4, 16, t), F32),
            vm((nch, t, CC), F32),
            vm((2, t, CC), F32),
            vm((nch, t, CC), F32),
            vm((nch, t, CC), F32),
            vm((t, CC), F32),
            vm((t, CC), F32),
            vm((t, CC), F32),
            dma((NA, 2)), dma((NB, EB)), dma((UC,)), dma((8,)), dma((nch,)),
            dma((3,)), dma((3,)),
            dma((UC,)), dma((UC,)), dma((UC,)), dma((UC,)), dma((UC,)), dma((UC,)),
            dma((nch,)), dma((nch,)), dma((nch,)), dma((nch,)), dma((nch,)), dma((nch,)),
        ],
        compiler_params=pltpu.CompilerParams(collective_id=0, has_side_effects=True,
                                             vmem_limit_bytes=67043328),
        name='moe_layer',
    )


def solution(mesh):
    g_ = mesh.shape['ep']
    rows = P(('dp', 'ep'))
    rep = P()

    def local(h0, idx, slot, ln_attn, wq, wk, wv, wo, ln_ffn, ws1, ws3, ws2, ln_moe, wr, ue1, ue3, ue2):
        b, s, d = h0.shape
        top = idx.shape[-1]
        el, _, fe = ue1.shape
        t = b * s
        cap = CAP_FACTOR * t * top // (el * g_)
        cos, sin = _rope_tables(s)
        gains = [w.reshape(d // 128, 128) for w in (ln_attn, ln_ffn, ln_moe)]
        ids = [jnp.transpose(a, (2, 0, 1)).reshape(top, 1, t) for a in (idx, slot)]
        call = _build(t, d, fe, ws1.shape[1], el, cap, top)
        out = call(h0.reshape(t, d), *ids, *gains, cos, sin, wr.T,
                   wq, wk, wv, wo, ws1, ws3, ws2, ue1, ue3, ue2)
        return out.reshape(b, s, d)

    specs = (rows, rows, rows) + (rep,) * 11 + (P('ep'), P('ep'), P('ep'))
    return jax.shard_map(local, mesh=mesh, in_specs=specs, out_specs=rows, check_vma=False)
```

```python
import jax
import jax.numpy as jnp
import numpy as np
from jax import lax
from jax.experimental import pallas as pl
from jax.experimental.pallas import tpu as pltpu
from jax.sharding import PartitionSpec as P

MESH = pl.DeviceIdType.MESH
F32 = jnp.float32
BF16 = jnp.bfloat16
EPS = 1e-6
HEAD = 128
CAP_FACTOR = 2

OWN, SIB, CROSS, DIAG = range(4)
NA = 4
NB = 4
EB = 4
CC = 256
UC = 4


def _dot(a, b):
    return jnp.dot(a, b, preferred_element_type=F32)


def _rope_tables(s):
    half = HEAD // 2
    freq = np.float32(10000.0) ** (-np.arange(half, dtype=np.float32) / np.float32(half))
    ang = np.arange(s, dtype=np.float32)[:, None] * freq.astype(np.float32)[None, :]
    c, sn = np.cos(ang), np.sin(ang)
    return np.concatenate([c, c], 1).astype(np.float32), np.concatenate([-sn, sn], 1).astype(np.float32)


def _build(t, d, fe, fs, el, cap, top):
    nh = d // HEAD
    rows = 4 * cap
    rl = el * cap
    nch = d // CC
    uc = t // UC
    nta = 8 + 2 * el
    nue2 = nch * el // EB
    dh = d // 2
    fh = fe // 2 // 256 * 256 + 256
    nf = fs // fe
    cpt = EB // nf
    nws2 = nch // cpt
    assert el == NB * EB and nws2 == NB

    def kernel(h0_hbm, idx_hbm, slot_hbm, lna_hbm, lnf_hbm, lnm_hbm, cos_hbm, sin_hbm, wr_hbm, wq, wk, wv, wo, ws1, ws3, ws2,
               ue1, ue3, ue2, out_hbm,
               idx_ref, slot_ref, gain_ref,
               ring_a, ring_b, u_all, comb, xbuf, ybuf, he, ln_ref, h0v, mrow,
               macc, rsib, rcross, rdiag, sdiag, ssib, pcs,
               sem_a, sem_b, sem_in, sem_small, sem_out,
               ms, mr, us_sib, ur_sib, us_cross, ur_cross, us_fwd, ur_diag,
               cs_diag, cr_diag, cs_sib, cr_sib, cs_cross, cr_cross):
        me = lax.axis_index('ep')
        core = lax.rem(me, 2)
        sib = me + 1 - 2 * core
        cross = lax.rem(me + 2, 4)
        diag = lax.rem(sib + 2, 4)
        base = (me * rl).astype(F32)

        def rcopy(src, dst, ssem, rsem, dev):
            return pltpu.make_async_remote_copy(src_ref=src, dst_ref=dst, send_sem=ssem, recv_sem=rsem,
                                                device_id={'ep': dev}, device_id_type=MESH)

        def a_dense(k):
            w = (wq, wk, wv, wo)[k // 2]
            return pltpu.make_async_copy(w.at[:, pl.ds((k % 2) * (d // 2), d // 2)],
                                         ring_a.at[k % NA, :, pl.ds(0, d // 2)], sem_a.at[k % NA, 0])

        def a_expert(e, s, h):
            cols = pl.ds(h * fh, (fh, fe - fh)[h])
            return pltpu.make_async_copy((ue1, ue3)[s % 2].at[e, :, cols], ring_a.at[s, :, cols], sem_a.at[s, h])

        def a_shared(k):
            return pltpu.make_async_copy((ws1, ws3)[k % 2].at[:, pl.ds((k // 2) * fe, fe)],
                                         ring_a.at[k], sem_a.at[k, 0])

        def b_ue2(i, sl):
            e0 = lax.rem(i, el // EB) * EB
            col = pl.multiple_of(lax.div(i, el // EB) * CC, CC)
            return pltpu.make_async_copy(ue2.at[pl.ds(e0, EB), :, pl.ds(col, CC)], ring_b.at[sl], sem_b.at[sl, 0])

        def b_ws2(i, sl):
            k = i - nue2
            return [pltpu.make_async_copy(
                ws2.at[pl.ds(half * fe, fe), pl.ds(pl.multiple_of((k * cpt + u) * CC, CC), CC)],
                ring_b.at[sl, u * nf + half], sem_b.at[sl, u * nf + half])
                for u in range(cpt) for half in range(nf)]

        h0_in = [pltpu.make_async_copy(h0_hbm.at[pl.ds(i * uc, uc)], h0v.at[pl.ds(i * uc, uc)], sem_in.at[i])
                 for i in range(UC)]
        small = [pltpu.make_async_copy(a, b, sem_small.at[i]) for i, (a, b) in enumerate((
            (lna_hbm, gain_ref.at[0]), (lnf_hbm, gain_ref.at[1]), (lnm_hbm, gain_ref.at[2]), (idx_hbm, idx_ref),
            (slot_hbm, slot_ref), (wr_hbm, xbuf.at[pl.ds(0, el * 4)]), (cos_hbm, macc.at[4, :, pl.ds(0, HEAD)]),
            (sin_hbm, macc.at[5, :, pl.ds(0, HEAD)])))]
        for cp in small[:3] + h0_in + small[3:]:
            cp.start()
        bar = pltpu.get_barrier_semaphore()
        for dev in (sib, cross, diag):
            pl.semaphore_signal(bar, inc=1, device_id={'ep': dev}, device_id_type=MESH)
        for k in range(3):
            small[k].wait()
        for k in range(3):
            w = gain_ref[k].astype(F32)
            for i in range(d // 128):
                ln_ref[k:k + 1, i * 128:(i + 1) * 128] = w[i:i + 1, :]

        def u_sib(i):
            r = pl.ds(i * uc, uc)
            return rcopy(u_all.at[OWN, r], u_all.at[SIB, r], us_sib.at[i], ur_sib.at[i], sib)

        def u_cross(i):
            r = pl.ds(i * uc, uc)
            return rcopy(u_all.at[OWN, r], u_all.at[CROSS, r],
                         us_cross.at[i], ur_cross.at[i], cross)

        def u_fwd(i):
            r = pl.ds(i * uc, uc)
            return rcopy(u_all.at[CROSS, r], u_all.at[DIAG, r],
                         us_fwd.at[i], ur_diag.at[i], sib)

        def relay(i):
            u_cross(i).wait_recv()
            u_fwd(i).start()

        def norm_in(k, _):
            r = pl.ds(pl.multiple_of(k * 16, 16), 16)
            x = h0v[r, :].astype(F32)
            n = x * lax.rsqrt(jnp.mean(x * x, axis=-1, keepdims=True) + EPS)
            u_all[OWN, r, :] = (n * ln_ref[2:3, :]).astype(BF16)
            x1 = (n * ln_ref[0:1, :]).astype(BF16)
            for half in range(2):
                he[pl.ds(pl.multiple_of((6 + half) * t + k * 16, 16), 16), 0:dh] = x1[:, half * dh:(half + 1) * dh]
            return 0

        def halves(k):
            return jnp.concatenate([he[k * t:(k + 1) * t, 0:dh], he[(k + 1) * t:(k + 2) * t, 0:dh]], axis=1)

        for i in range(UC):
            h0_in[i].wait()
            if i == 1:
                for k in range(NA):
                    a_dense(k).start()
            lax.fori_loop(i * uc // 16, (i + 1) * uc // 16, norm_in, 0)
            if i == 0:
                pl.semaphore_wait(bar, 3)
            if i < UC // 2:
                u_cross(i).start()
                u_sib(i).start()
        for k in range(3, 8):
            small[k].wait()

        lg = lax.dot_general(xbuf[0:el * 4, :], u_all[OWN], (((1,), (1,)), ((), ())), preferred_element_type=F32)
        ex = lax.broadcasted_iota(jnp.int32, lg.shape, 0)
        lj = [jnp.sum(jnp.where(ex == idx_ref[j], lg, 0.0), axis=0, keepdims=True) for j in range(top)]
        mx = lj[0]
        for j in range(1, top):
            mx = jnp.maximum(mx, lj[j])
        ej = [jnp.exp(v - mx) for v in lj]
        tot = ej[0]
        for j in range(1, top):
            tot = tot + ej[j]
        mrow[OWN] = jnp.zeros((16, t), F32)
        for j in range(top):
            mrow[OWN, j:j + 1, :] = (idx_ref[j] * cap + slot_ref[j]).astype(F32)
            mrow[OWN, 8 + j:9 + j, :] = ej[j] / tot
        m_sib, m_cross, m_fwd = [rcopy(mrow.at[a], mrow.at[b], ms.at[b - 1], mr.at[b - 1], dev)
                                 for a, b, dev in ((OWN, SIB, sib), (OWN, CROSS, cross), (CROSS, DIAG, sib))]
        m_cross.start()
        m_sib.start()
        for i in range(UC // 2, UC):
            u_cross(i).start()
            u_sib(i).start()

        def qkv(k, rope):
            a_dense(k).wait()

            for n in range(2):
                y = _dot(halves(6), ring_a[k % NA, :, n * 512:(n + 1) * 512])
                for h in range(4):
                    yh = y[:, h * HEAD:(h + 1) * HEAD]
                    if rope:
                        yh = yh * macc[4, :, 0:HEAD] + pltpu.roll(yh, HEAD // 2, 1) * macc[5, :, 0:HEAD]
                    col = n * 512 + h * HEAD
                    he[k * t:(k + 1) * t, col:col + HEAD] = yh.astype(BF16)

        for k in range(6):
            qkv(k, k < 4)
            if k < 4:
                a_dense(k + NA).start()
            else:
                a_expert(0, k % NA, 0).start()
                a_expert(0, k % NA, 1).start()
        relay(0)
        for i in range(NB):
            b_ue2(i, i).start()

        ri = lax.broadcasted_iota(jnp.int32, (t, t), 0)
        ci = lax.broadcasted_iota(jnp.int32, (t, t), 1)

        def head_pair(hp, _):
            for s in range(2):
                half = lax.div(hp, nh // 4)
                col = pl.ds(pl.multiple_of((lax.rem(hp, nh // 4) * 2 + s) * HEAD, HEAD), HEAD)
                rq, rk, rv = (pl.ds(pl.multiple_of((2 * kind + half) * t, t), t) for kind in range(3))
                q = he[rq, col]
                kk = he[rk, col]
                vv = he[rv, col]
                sc = lax.dot_general(q, kk, (((1,), (1,)), ((), ())), preferred_element_type=F32) * HEAD ** -0.5
                sc = jnp.where(ri >= ci, sc, -1e30)
                p = jnp.exp(sc - jnp.max(sc, axis=-1, keepdims=True))
                p = (p / jnp.sum(p, axis=-1, keepdims=True)).astype(BF16)
                he[rq, col] = _dot(p, vv).astype(BF16)
            return 0

        lax.fori_loop(0, nh // 2, head_pair, 0)
        m_cross.wait_recv()
        m_fwd.start()
        relay(1)

        def onehot(e, role):
            rr = (lax.broadcasted_iota(jnp.int32, (cap, t), 0) + e * cap).astype(F32) + base
            hit = rr == mrow[role, 0:1, :]
            for j in range(1, top):
                hit = hit | (rr == mrow[role, j:j + 1, :])
            return jnp.where(hit, 1.0, 0.0).astype(BF16)

        def gather(e, buf, role):
            oh = onehot(e, role)
            r0 = buf * rows + role * cap
            for n in range(d // 512):
                xbuf[r0:r0 + cap, n * 512:(n + 1) * 512] = _dot(oh, u_all[role, :, n * 512:(n + 1) * 512]).astype(BF16)

        def gather_first(role):
            oh = jnp.concatenate([onehot(0, role)] + [onehot(2 * p + 1, role) for p in range(el // 2)], axis=0)
            for n in range(d // 512):
                x = _dot(oh, u_all[role, :, n * 512:(n + 1) * 512]).astype(BF16)
                xbuf[role * cap:(role + 1) * cap, n * 512:(n + 1) * 512] = x[0:cap, :]
                half, col = divmod(n * 512, dh)
                for p in range(el // 2):
                    r0 = (2 * p + half) * rows + role * cap
                    he[r0:r0 + cap, col:col + 512] = x[(p + 1) * cap:(p + 2) * cap, :]

        for k in (6, 7):
            a_dense(k).wait()

            for n in range(2):
                col = slice((k % 2) * (d // 2) + n * 512, (k % 2) * (d // 2) + (n + 1) * 512)
                y = _dot(halves(0), ring_a[k % NA, :, n * 512:(n + 1) * 512])
                h0v[:, col] = (h0v[:, col].astype(F32) + y).astype(BF16)
            a_expert(1, k % NA, 0).start()
            a_expert(1, k % NA, 1).start()

        m_sib.wait()
        m_cross.wait_send()
        m_fwd.wait()
        for role in range(4):
            macc[role, :, 0:128] = jnp.transpose(jnp.concatenate([mrow[role], jnp.zeros((112, t), F32)], axis=0))
        for i in range(2, UC - 1):
            relay(i)
        for i in range(UC):
            u_sib(i).wait()
        gather_first(OWN)
        gather_first(SIB)
        relay(UC - 1)
        for sl in range(NB):
            b_ue2(sl, sl).wait()

        def swiglu(lhs, sl, dr, between=()):
            between = list(between)
            for n0 in range(0, fe - fe % 256, 256):
                cols = slice(n0, n0 + 256)
                y1 = _dot(lhs(), ring_a[sl, :, cols])
                y3 = _dot(lhs(), ring_a[sl + 1, :, cols])
                he[dr, cols] = (y1 * jax.nn.sigmoid(y1) * y3).astype(BF16)
                if between:
                    between.pop(0)()
            if fe % 256:
                cols = slice(fe - fe % 256, fe)
                y = sum(_dot(lhs()[:, k:k + dh], jnp.concatenate(
                    [ring_a[sl, k:k + dh, cols], ring_a[sl + 1, k:k + dh, cols]], axis=1)) for k in (0, dh))
                y1, y3 = y[:, :fe % 256], y[:, fe % 256:]
                he[dr, cols] = (y1 * jax.nn.sigmoid(y1) * y3).astype(BF16)

        npart = 4 * t // el
        def gate_part(i):
            role = lax.div(i, el // 4)
            r = pl.ds(pl.multiple_of(lax.rem(i, el // 4) * npart, npart), npart)
            for b in range(rl // 256):
                rr = (lax.broadcasted_iota(jnp.int32, (npart, 256), 1) + b * 256).astype(F32) + base
                w = jnp.zeros((npart, 256), F32)
                for j in range(top):
                    w = jnp.where(rr == macc[role, r, j:j + 1], macc[role, r, 8 + j:9 + j], w)
                for part in range(3):
                    piece = w.astype(BF16)
                    comb[role, r, part * rl + b * 256:part * rl + (b + 1) * 256] = piece
                    w = w - piece.astype(F32)

        gather_first(CROSS)
        for i in range(UC):
            u_cross(i).wait_send()
            u_fwd(i).wait()
        gather_first(DIAG)

        def y_first(e):
            er = pl.ds(pl.multiple_of(e * rows, 16), rows)
            y = sum(_dot(he[er, a:b], ring_b[lax.div(e, EB), lax.rem(e, EB), a:b, :])
                    for a, b in ((0, fh), (fh, fe))).astype(BF16)
            for role in range(4):
                ybuf[pl.ds(pl.multiple_of(e * cap, 16), cap), role * CC:(role + 1) * CC] = y[role * cap:(role + 1) * cap, :]

        def expert(e, s, last):
            sls = (2 * s, 2 * s + 1)
            for h in range(2):
                for sl in sls:
                    a_expert(e, sl, h).wait()
            if s == 0:
                for half in range(2):
                    xbuf[rows:2 * rows, half * dh:(half + 1) * dh] = (
                        he[pl.ds(pl.multiple_of((e + half) * rows, 16), rows), 0:dh])
            y_first(e - 1 if isinstance(e, int) else jnp.maximum(e - 1, 0))
            gate_part(e)

            def refill(h):
                for sl in sls:
                    a_expert(e + 2, sl, h).start()

            def step(k):
                if s == 1 and not last:
                    gather(e + 1, 0, k)
                if (k + 1) * 256 == fh and not last:
                    refill(0)

            swiglu(lambda: xbuf[s * rows:(s + 1) * rows, :], 2 * s, pl.ds(pl.multiple_of(e * rows, 16), rows),
                   [lambda k=k: step(k) for k in range(4)])
            if not last:
                refill(1)

        def pair(p, _):
            for s in range(2):
                expert(p * 2 + s, s, False)
            return 0

        lax.fori_loop(0, el // 2 - 1, pair, 0)
        for sl in range(NB - 1):
            b_ue2(NB + sl, sl).start()
        for s in range(2):
            expert(el - 2 + s, s, True)

        def norm_a(c):
            nr = t // nch
            r = pl.ds(pl.multiple_of(c * nr, nr), nr)
            x = h0v[r, :].astype(F32)
            n = x * lax.rsqrt(jnp.mean(x * x, axis=-1, keepdims=True) + EPS)
            u_all[0, r, :] = (n * ln_ref[1:2, :]).astype(BF16)

        def c_diag(c):
            return rcopy(sdiag, rdiag.at[c], cs_diag.at[c], cr_diag.at[c], sib)

        def c_sib(c):
            return rcopy(ssib, rsib.at[lax.rem(c, 2)], cs_sib.at[c], cr_sib.at[c], sib)

        def c_cross(c):
            return rcopy(rdiag.at[c], rcross.at[c], cs_cross.at[c], cr_cross.at[c], cross)

        def partial(role):
            yc = ybuf[:, role * CC:(role + 1) * CC]
            return _dot(comb[role], jnp.concatenate([yc, yc, yc], axis=0))

        def exchange(c):
            sdiag[...] = partial(DIAG)
            ssib[...] = partial(SIB)
            c_diag(c).start()
            c_sib(c).start()
            pcs[...] = partial(CROSS)
            macc[c] = partial(OWN)

        def send_cross(c):
            c_diag(c).wait_recv()
            rdiag[c] = rdiag[c] + pcs[...]
            c_cross(c).start()

        def add_sib(c):
            c_sib(c).wait_recv()
            macc[c] = macc[c] + rsib[lax.rem(c, 2)]

        def chunk(c, _):
            @pl.when(c <= 2 * nf)
            def _():
                for k in range(2 * nf):
                    @pl.when(c == k + 1)
                    def _():
                        a_shared(k).start()

            for blk in range(2):
                slots = range(blk * (NB // 2), (blk + 1) * (NB // 2))
                for sl in slots:
                    b_ue2(c * NB + sl, sl).wait()
                if blk == 1:
                    norm_a(c)
                for sl in slots:
                    for s in range(EB):
                        e = sl * EB + s
                        y = _dot(he[e * rows:(e + 1) * rows, :], ring_b[sl, s]).astype(BF16)
                        for role in range(4):
                            ybuf[e * cap:(e + 1) * cap, role * CC:(role + 1) * CC] = y[role * cap:(role + 1) * cap, :]

                @pl.when(c + 1 < nch)
                def _():
                    for sl in slots:
                        b_ue2((c + 1) * NB + sl, sl).start()

                @pl.when(c + 1 == nch)
                def _():
                    for sl in slots:
                        for cp in b_ws2(nue2 + sl, sl):
                            cp.start()

                if blk == 0:
                    @pl.when(c >= 5)
                    def _():
                        send_cross(c - 1)

                    add_sib(c - 1)

            c_diag(c - 1).wait_send()
            c_sib(c - 1).wait_send()
            exchange(c)

            @pl.when((c <= 3) | (c == nch - 1))
            def _():
                send_cross(c)
            return 0

        y_first(el - 1)
        b_ue2(2 * NB - 1, NB - 1).start()
        exchange(0)
        send_cross(0)
        norm_a(0)
        lax.fori_loop(1, nch, chunk, 0)
        add_sib(nch - 1)

        for half in range(nf):
            a_shared(2 * half).wait()
            a_shared(2 * half + 1).wait()
            swiglu(lambda: u_all[0], 2 * half, slice(half * t, (half + 1) * t))

        for k in range(nws2):
            for cp in b_ws2(nue2 + k, k):
                cp.wait()

        def shared_out(k, _):
            for u in range(cpt):
                f = macc[k * cpt + u]
                for half in range(nf):
                    f = f + _dot(he[half * t:(half + 1) * t, :], ring_b[k, u * nf + half])
                macc[k * cpt + u] = f
            return 0

        lax.fori_loop(0, nws2, shared_out, 0)
        for c in range(nch):
            cols = slice(c * CC, (c + 1) * CC)
            c_cross(c).wait_recv()

            def fin(k, _):
                r = pl.ds(pl.multiple_of(k * 32, 32), 32)
                u_all[1, r, cols] = (h0v[r, cols].astype(F32) + macc[c, r] + rcross[c, r]).astype(BF16)
                return 0

            lax.fori_loop(0, t // 32, fin, 0)
            pltpu.make_async_copy(u_all.at[1, :, pl.ds(c * CC, CC)], out_hbm.at[:, pl.ds(c * CC, CC)],
                                  sem_out.at[c]).start()
        for c in range(nch):
            if c == nch - 1:
                c_diag(c).wait_send()
                c_sib(c).wait_send()
            c_cross(c).wait_send()
            pltpu.make_async_copy(u_all.at[1, :, pl.ds(c * CC, CC)], out_hbm.at[:, pl.ds(c * CC, CC)],
                                  sem_out.at[c]).wait()

    dma = pltpu.SemaphoreType.DMA
    vm = pltpu.VMEM
    any_ = pl.BlockSpec(memory_space=pl.ANY)
    return pl.pallas_call(
        kernel,
        out_shape=jax.ShapeDtypeStruct((t, d), BF16),
        in_specs=[any_] * 19,
        out_specs=any_,
        scratch_shapes=[
            vm((top, 1, t), jnp.int32), vm((top, 1, t), jnp.int32),
            vm((3, d // 128, 128), BF16),
            vm((NA, d, fe), BF16),
            vm((NB, EB, fe, CC), BF16),
            vm((4, t, d), BF16),
            vm((4, t, 3 * rl), BF16),
            vm((2 * rows, d), BF16),
            vm((rl, 4 * CC), BF16),
            vm((el * rows, fe), BF16),
            vm((8, d), F32),
            vm((t, d), BF16),
            vm((4, 16, t), F32),
            vm((nch, t, CC), F32),
            vm((2, t, CC), F32),
            vm((nch, t, CC), F32),
            vm((nch, t, CC), F32),
            vm((t, CC), F32),
            vm((t, CC), F32),
            vm((t, CC), F32),
            dma((NA, 2)), dma((NB, EB)), dma((UC,)), dma((8,)), dma((nch,)),
            dma((3,)), dma((3,)),
            dma((UC,)), dma((UC,)), dma((UC,)), dma((UC,)), dma((UC,)), dma((UC,)),
            dma((nch,)), dma((nch,)), dma((nch,)), dma((nch,)), dma((nch,)), dma((nch,)),
        ],
        compiler_params=pltpu.CompilerParams(collective_id=0, has_side_effects=True,
                                             vmem_limit_bytes=67043328),
        name='moe_layer',
    )


def solution(mesh):
    g_ = mesh.shape['ep']
    rows = P(('dp', 'ep'))
    rep = P()

    def local(h0, idx, slot, ln_attn, wq, wk, wv, wo, ln_ffn, ws1, ws3, ws2, ln_moe, wr, ue1, ue3, ue2):
        b, s, d = h0.shape
        top = idx.shape[-1]
        el, _, fe = ue1.shape
        t = b * s
        cap = CAP_FACTOR * t * top // (el * g_)
        cos, sin = _rope_tables(s)
        gains = [w.reshape(d // 128, 128) for w in (ln_attn, ln_ffn, ln_moe)]
        ids = [jnp.transpose(a, (2, 0, 1)).reshape(top, 1, t) for a in (idx, slot)]
        call = _build(t, d, fe, ws1.shape[1], el, cap, top)
        out = call(h0.reshape(t, d), *ids, *gains, cos, sin, wr.T,
                   wq, wk, wv, wo, ws1, ws3, ws2, ue1, ue3, ue2)
        return out.reshape(b, s, d)

    specs = (rows, rows, rows) + (rep,) * 11 + (P('ep'), P('ep'), P('ep'))
    return jax.shard_map(local, mesh=mesh, in_specs=specs, out_specs=rows, check_vma=False)
```
